256 devices in a mesh: gx: 16 (over x_lo, y, core), gy: 16 (over z, x_hi).
Axes of the slice: x: 4 (x_hi: 2, x_lo: 2; x = x_hi * 2 + x_lo), y: 4, z: 8, core: 2. Of those that a mesh axis runs over, the one named last changes fastest.
Arguments:
- source: float32 [320, 320, 640], P('gx', 'gy'), may hold values from -210 to 210
- conductivity: float32 [320, 320, 640], P('gx', 'gy'), may hold values from 0.001 to 1
- absorption: float32 [320, 320, 640], P('gx', 'gy'), may hold values from 1 to 10
Outputs:
- solution: float32 [320, 320, 640], P('gx', 'gy')
- correction: float32 [192, 192, 384], P('gx', 'gy')
The draws below stay inside these ranges and needn't reach their ends.
All inputs are finite; a program needn't handle non-finite values.
Results may differ from the reference program's by a relative error of at most 0.00023.
Values sent between devices are 32-bit elements; how exact they have to be, the bound alone decides.
A program may use at most 128 MiB of HBM per device.

```python
import math
import jax
import jax.numpy as jnp
import numpy as np
from jax import lax

SWEEPS = 3
NX = 320
NY = 320
NZ = 640


def draw_source(key, part):
    first = jax.random.fold_in(key, 0)
    shape = (NX, NY, NZ)
    rise_x = 3.0 ** (jnp.arange(NX, dtype=jnp.float32) / NX)
    rise_y = 3.0 ** (jnp.arange(NY, dtype=jnp.float32) / NY)
    ramp = rise_x[:, None, None] * rise_y[None, :, None]
    base = jax.random.truncated_normal(first, -4.0, 4.0, shape, jnp.float32)
    return (base * ramp).astype(jnp.float32)


def draw_conductivity(key, part):
    inner = jax.random.fold_in(key, 17)
    shape = (NX, NY, NZ)
    place_x = jnp.arange(NX, dtype=jnp.float32) / NX
    place_y = jnp.arange(NY, dtype=jnp.float32) / NY
    rise_x = 10.0 ** place_x / 10.0
    base = jnp.exp(jax.random.uniform(inner, shape, jnp.float32, math.log(0.1), 0.0))
    rise_y = 3.0 ** place_y / 3.0
    ramp = rise_x[:, None, None] * rise_y[None, :, None]
    return (base * ramp).astype(jnp.float32)


def levels(stream_key, dims, cuts, low, largest):
    gain, own = 1.0, jax.random.fold_in(stream_key, 6)
    for position, blocks in cuts:
        steps = jnp.exp(jax.random.uniform(jax.random.fold_in(own, position), (blocks,), jnp.float32, low / len(cuts), largest / len(cuts)))
        gain = gain * jnp.repeat(steps, dims[position] // blocks).reshape([-1 if axis == position else 1 for axis in range(len(dims))])
    return gain


def setup_inputs(seed: int = 0) -> dict:
    splits = jax.random.split(jax.random.key(seed), 4)
    return {
        "source": draw_source(jax.random.fold_in(splits[3], 71), 0),
        "conductivity": draw_conductivity(jax.random.fold_in(splits[3], 71), 0),
        "absorption": jnp.clip(jnp.exp(math.log(10.0) - 2.3025851 * jax.random.uniform(splits[2], (NX, NY, NZ), jnp.float32) ** levels(splits[2], (NX, NY, NZ), ((0, 16), (1, 16)), -0.2, 0.2)), 1.0, 10.0),
    }


HIGH = lax.Precision.HIGHEST

def deriv_table(points):
    count = len(points)
    barycentric = np.array([1.0 / np.prod([points[j] - points[k] for k in range(count) if k != j]) for j in range(count)])
    table = np.zeros((count, count))
    for i in range(count):
        for j in range(count):
            if i != j:
                table[i, j] = barycentric[j] / (barycentric[i] * (points[i] - points[j]))
        table[i, i] = -np.sum(table[i])
    return table

def make_tables():
    root = math.sqrt(3.0 / 7.0)
    fine_points = np.array([-1.0, -root, 0.0, root, 1.0])
    fine_weights = np.array([0.1, 49.0 / 90.0, 32.0 / 45.0, 49.0 / 90.0, 0.1])
    coarse_points = np.array([-1.0, 0.0, 1.0])
    coarse_weights = np.array([1.0 / 3.0, 4.0 / 3.0, 1.0 / 3.0])
    interp = np.stack([fine_points * (fine_points - 1.0) / 2.0, 1.0 - fine_points ** 2, fine_points * (fine_points + 1.0) / 2.0], 1)
    select = np.zeros((3, 5))
    select[0, 0] = 1.0
    select[1, 2] = 1.0
    select[2, 4] = 1.0
    return [jnp.asarray(t, jnp.float32) for t in (fine_weights, coarse_weights, deriv_table(fine_points), deriv_table(coarse_points), interp, select)]

def along(field, table, axis):
    count_out, count_in = table.shape
    shape = field.shape
    elems = shape[axis] // count_in
    split = field.reshape(shape[:axis] + (elems, count_in) + shape[axis + 1:])
    moved = jnp.moveaxis(split, axis + 1, -1)
    mixed = jnp.einsum('...i,pi->...p', moved, table, precision=HIGH)
    back = jnp.moveaxis(mixed, -1, axis + 1)
    return back.reshape(shape[:axis] + (elems * count_out,) + shape[axis + 1:])

def end_masks(length, count, axis):
    index = jnp.arange(length) % count
    shape = [1, 1, 1]
    shape[axis] = length
    return ((index == 0).reshape(shape), (index == count - 1).reshape(shape))

def assemble(field, count):
    for axis in range(3):
        lower, upper = end_masks(field.shape[axis], count, axis)
        field = field + jnp.where(upper, jnp.roll(field, -1, axis), 0.0) + jnp.where(lower, jnp.roll(field, 1, axis), 0.0)
    return field

def node_weights(shape, weights):
    count = weights.shape[0]
    first = jnp.tile(weights, shape[0] // count)
    second = jnp.tile(weights, shape[1] // count)
    third = jnp.tile(weights, shape[2] // count)
    return first[:, None, None] * second[None, :, None] * third[None, None, :]

def half_ends(shape, count):
    parts = []
    for axis in range(3):
        lower, upper = end_masks(shape[axis], count, axis)
        parts.append(jnp.where(lower | upper, 0.5, 1.0))
    return parts[0] * parts[1] * parts[2]

def local_op(field, flux, mass, deriv):
    result = mass * field
    for axis in range(3):
        result = result + along(flux * along(field, deriv, axis), deriv.T, axis)
    return result

def local_diag(flux, mass, deriv):
    result = mass
    square = (deriv * deriv).T
    for axis in range(3):
        result = result + along(flux, square, axis)
    return result

def chebyshev(rhs, apply, inverse, estimate, want_residual):
    theta = 0.75 * estimate
    delta = 0.45 * estimate
    sigma = 5.0 / 3.0
    rho = 0.6
    solution = jnp.zeros_like(rhs)
    residual = rhs
    direction = inverse * residual / theta
    for sweep in range(SWEEPS):
        solution = solution + direction
        if sweep + 1 < SWEEPS or want_residual:
            residual = residual - apply(direction)
        if sweep + 1 < SWEEPS:
            rho_next = 1.0 / (2.0 * sigma - rho)
            direction = rho_next * rho * direction + 2.0 * rho_next / delta * inverse * residual
            rho = rho_next
    return (solution, residual)

def estimate_of(start, apply, inverse):
    first = inverse * apply(start)
    second = inverse * apply(first)
    return jnp.sqrt(jnp.sum(second * second) / (jnp.sum(first * first) + 1e-06))

def reference(source, conductivity, absorption):
    fine_weights, coarse_weights, fine_deriv, coarse_deriv, interp, select = make_tables()
    fine_w = node_weights(source.shape, fine_weights)
    fine_flux = fine_w * conductivity
    fine_mass = fine_w * absorption

    def apply_fine(field):
        return assemble(local_op(field, fine_flux, fine_mass, fine_deriv), 5)
    load = assemble(fine_w * source, 5)
    fine_inverse = 1.0 / assemble(local_diag(fine_flux, fine_mass, fine_deriv), 5)
    fine_estimate = estimate_of(load, apply_fine, fine_inverse)
    smoothed, fine_residual = chebyshev(load, apply_fine, fine_inverse, fine_estimate, True)
    coarse_cond = conductivity
    coarse_abs = absorption
    for axis in range(3):
        coarse_cond = along(coarse_cond, select, axis)
        coarse_abs = along(coarse_abs, select, axis)
    coarse_w = node_weights(coarse_cond.shape, coarse_weights)
    coarse_flux = coarse_w * coarse_cond
    coarse_mass = coarse_w * coarse_abs
    halves = half_ends(source.shape, 5)

    def apply_coarse(field):
        return assemble(local_op(field, coarse_flux, coarse_mass, coarse_deriv), 3)

    def restrict(field):
        field = field * halves
        for axis in range(3):
            field = along(field, interp.T, axis)
        return assemble(field, 3)
    coarse_inverse = 1.0 / assemble(local_diag(coarse_flux, coarse_mass, coarse_deriv), 3)
    coarse_estimate = estimate_of(restrict(load), apply_coarse, coarse_inverse)
    correction, unused = chebyshev(restrict(fine_residual), apply_coarse, coarse_inverse, coarse_estimate, False)
    lifted = correction
    for axis in range(3):
        lifted = along(lifted, interp, axis)
    return (smoothed + lifted, correction)
```

```python
import functools
import math

import jax
import jax.numpy as jnp
import numpy as np
from jax import lax
from jax.experimental import pallas as pl
from jax.experimental.pallas import tpu as pltpu
from jax.sharding import PartitionSpec as P

MESH = pl.DeviceIdType.MESH
SWEEPS = 3
F32 = jnp.float32


def deriv_table(points):
    count = len(points)
    bary = [1.0 / np.prod([points[j] - points[k] for k in range(count) if k != j]) for j in range(count)]
    table = np.zeros((count, count))
    for i in range(count):
        for j in range(count):
            if i != j:
                table[i, j] = bary[j] / (bary[i] * (points[i] - points[j]))
        table[i, i] = -np.sum(table[i])
    return table


ROOT = math.sqrt(3.0 / 7.0)
WF = [0.1, 49.0 / 90.0, 32.0 / 45.0, 49.0 / 90.0, 0.1]
WC = [1.0 / 3.0, 4.0 / 3.0, 1.0 / 3.0]
DF = deriv_table(np.array([-1.0, -ROOT, 0.0, ROOT, 1.0]))
JA, JB, JC = (ROOT * ROOT + ROOT) / 2, 1 - ROOT * ROOT, (ROOT * ROOT - ROOT) / 2
JROWS = [[1.0, 0.0, 0.0], [JA, JB, JC], [0.0, 1.0, 0.0], [JC, JB, JA], [0.0, 0.0, 1.0]]


B00, B01 = (DF[4][4] + DF[0][4]) / 2, (DF[4][3] + DF[0][3]) / 2
B10, B11 = (DF[3][4] + DF[1][4]) / 2, (DF[3][3] + DF[1][3]) / 2
G00, G01 = (DF[4][4] - DF[0][4]) / 2, (DF[4][3] - DF[0][3]) / 2
G10, G11 = (DF[3][4] - DF[1][4]) / 2, (DF[3][3] - DF[1][3]) / 2
A0, A1 = DF[2][4], DF[2][3]


def stiff5(v, flux):
    a0, a1 = v[4] - v[0], v[3] - v[1]
    m2 = v[2] + v[2]
    s0, s1 = v[0] + v[4] - m2, v[1] + v[3] - m2
    p0, p1 = B00 * a0 + B01 * a1, B10 * a0 + B11 * a1
    q0, q1 = G00 * s0 + G01 * s1, G10 * s0 + G11 * s1
    f0, f4 = flux[0] * (p0 - q0), flux[4] * (p0 + q0)
    f1, f3 = flux[1] * (p1 - q1), flux[3] * (p1 + q1)
    f2 = flux[2] * (A0 * a0 + A1 * a1)
    sp0, sq0, sp1, sq1 = f4 + f0, f4 - f0, f3 + f1, f3 - f1
    b0 = A0 * f2 + B00 * sp0 + B10 * sp1
    b1 = A1 * f2 + B01 * sp0 + B11 * sp1
    c0, c1 = G00 * sq0 + G10 * sq1, G01 * sq0 + G11 * sq1
    mid = c0 + c1
    return [c0 - b0, c1 - b1, -(mid + mid), c1 + b1, c0 + b0]


DD = (DF * DF).T


def diag5(flux):
    s0, s1, d0, d1 = flux[0] + flux[4], flux[1] + flux[3], flux[0] - flux[4], flux[1] - flux[3]
    out = [None] * 5
    for r in (0, 1):
        even = (DD[r][0] + DD[r][4]) / 2 * s0 + (DD[r][1] + DD[r][3]) / 2 * s1 + DD[r][2] * flux[2]
        odd = (DD[r][0] - DD[r][4]) / 2 * d0 + (DD[r][1] - DD[r][3]) / 2 * d1
        out[r], out[4 - r] = even + odd, even - odd
    out[2] = DD[2][0] * s0 + DD[2][1] * s1
    return out


def stiff3(v, flux):
    a = 0.5 * (v[2] - v[0])
    s = v[0] + v[2] - (v[1] + v[1])
    f0, f1, f2 = flux[0] * (a - s), flux[1] * a, flux[2] * (a + s)
    b = 0.5 * (f0 + f1 + f2)
    t = f2 - f0
    return [t - b, -(t + t), t + b]


DC = deriv_table(np.array([-1.0, 0.0, 1.0]))
DDC = (DC * DC).T


def diag3(flux):
    s = flux[0] + flux[2]
    return [
        DDC[0][0] * flux[0] + DDC[0][1] * flux[1] + DDC[0][2] * flux[2],
        DDC[1][0] * s,
        DDC[2][0] * flux[0] + DDC[2][1] * flux[1] + DDC[2][2] * flux[2],
    ]


def restrict5(y):
    return [y[0] + JA * y[1] + JC * y[3], JB * (y[1] + y[3]) + y[2], y[4] + JC * y[1] + JA * y[3]]


def up(x):
    return pltpu.roll(x, 127, 1)


def down(x):
    return pltpu.roll(x, 1, 1)


def loop(count, body, unroll=1):
    def step(i, carry):
        body(i)
        return carry

    lax.fori_loop(0, count, step, 0, unroll=unroll)


class Level:
    def __init__(self, q, fxy, f0, fq, mass, inv):
        self.q, self.kz = q, q - 1
        self.fxy, self.f0, self.fq, self.mass, self.inv = fxy, f0, fq, mass, inv
        self.stiff, self.diag = (stiff5, diag5) if q == 5 else (stiff3, diag3)
        self.face = q * self.kz * 4
        self.loop = loop if q == 5 else (lambda n, body: [body(i) for i in range(n)])

    def at(self, i, j, k):
        return ((i * self.q + j) * self.kz + k) * 16

    def edge(self, i, j):
        return (i * self.q + j) * 16


def row(ref, start):
    if not isinstance(start, int):
        start = pl.multiple_of(start, 16)
    return ref[pl.ds(start, 16), :]


def put(ref, start, value):
    if not isinstance(start, int):
        start = pl.multiple_of(start, 16)
    ref[pl.ds(start, 16), :] = value


def element_rows():
    e = lax.broadcasted_iota(jnp.int32, (16, 128), 0)
    return e // 4, e % 4


def join_y(lo, hi):
    _, ey = element_rows()
    hi = hi + jnp.where(ey < 3, pltpu.roll(lo, 15, 0), 0.0)
    return jnp.where(ey > 0, pltpu.roll(hi, 1, 0), lo), hi


def join_x(lo, hi):
    ex, _ = element_rows()
    hi = hi + jnp.where(ex < 3, pltpu.roll(lo, 12, 0), 0.0)
    return jnp.where(ex > 0, pltpu.roll(hi, 4, 0), lo), hi


def join_planes_x(lv, out):
    q, kz = lv.q, lv.kz

    def body(j):
        for k in range(kz):
            lo, hi = join_x(row(out, lv.at(0, j, k)), row(out, lv.at(q - 1, j, k)))
            put(out, lv.at(0, j, k), lo)
            put(out, lv.at(q - 1, j, k), hi)

    lv.loop(q, body)


def join_planes_y(lv, out):
    q, kz = lv.q, lv.kz

    def body(i):
        for k in range(kz):
            lo, hi = join_y(row(out, lv.at(i, 0, k)), row(out, lv.at(i, q - 1, k)))
            put(out, lv.at(i, 0, k), lo)
            put(out, lv.at(i, q - 1, k), hi)

    lv.loop(q, body)


def apply_local(lv, out, u, scaled=None, sums=None, restrict=None, keep=True):
    q, kz = lv.q, lv.kz

    def along_z(i):
        total = None
        for j in range(q):
            base = lv.at(i, j, 0)
            if scaled is None:
                v = [row(u, base + 16 * k) for k in range(kz)]
            else:
                v = [row(scaled, base + 16 * k) * row(lv.inv, base + 16 * k) for k in range(kz)]
                for k in range(kz):
                    put(u, base + 16 * k, v[k])
                if sums is not None:
                    part = v[0] * v[0]
                    part = part + part
                    for k in range(1, kz):
                        part = part + v[k] * v[k]
                    total = part if total is None else total + part
            flux = [row(lv.f0, lv.edge(i, j))] + [row(lv.fxy, base + 16 * k) for k in range(1, kz)] + [row(lv.fq, lv.edge(i, j))]
            g = lv.stiff(v + [up(v[0])], flux)
            g = [g[0] + down(g[kz])] + g[1:kz]
            for k in range(kz):
                put(out, base + 16 * k, g[k] + row(lv.mass, base + 16 * k) * v[k])
        if sums is not None:
            sums[...] += total

    def along_x(j):
        for k in range(kz):
            places = [lv.at(i, j, k) for i in range(q)]
            g = lv.stiff([row(u, p) for p in places], [row(lv.fxy, p) for p in places])
            for i in range(q):
                put(out, places[i], row(out, places[i]) + g[i])

    def along_y(i):
        for k in range(kz):
            places = [lv.at(i, j, k) for j in range(q)]
            g = lv.stiff([row(u, p) for p in places], [row(lv.fxy, p) for p in places])
            g = [row(out, places[j]) + g[j] for j in range(q)]
            if restrict is not None:
                c = restrict5(g)
                for jc in range(3):
                    put(restrict, ((i * 3 + jc) * 4 + k) * 16, c[jc])
            if keep:
                g[0], g[q - 1] = join_y(g[0], g[q - 1])
                for j in range(q):
                    put(out, places[j], g[j])

    if sums is not None:
        sums[...] = jnp.zeros_like(sums)
    lv.loop(q, along_z)
    lv.loop(q, along_x)
    lv.loop(q, along_y)
    if keep:
        join_planes_x(lv, out)


def sum_squares(lv, scaled, sums):
    sums[...] = jnp.zeros_like(sums)

    def body(i):
        total = None
        for j in range(lv.q):
            for k in range(lv.kz):
                p = lv.at(i, j, k)
                v = row(scaled, p) * row(lv.inv, p)
                v = v * v
                if k == 0:
                    v = v + v
                total = v if total is None else total + v
        sums[...] += total

    lv.loop(lv.q, body)


def restrict_xz(lc, tmp, out):
    for jc in range(3):
        cols = [restrict5([row(tmp, ((i * 3 + jc) * 4 + k) * 16) for i in range(5)]) for k in range(4)]
        for ic in range(3):
            y = [cols[k][ic] for k in range(4)]
            first = y[0] + JA * y[1] + JC * y[3] + down(JC * y[1] + JA * y[3])
            put(out, lc.at(ic, jc, 0), first)
            put(out, lc.at(ic, jc, 1), JB * (y[1] + y[3]) + y[2])
    join_planes_y(lc, out)
    join_planes_x(lc, out)


def restrict_y(lv, src, tmp):
    def body(i):
        for k in range(4):
            c = restrict5([row(src, lv.at(i, j, k)) for j in range(5)])
            for jc in range(3):
                put(tmp, ((i * 3 + jc) * 4 + k) * 16, c[jc])

    loop(5, body)


def local_diag(lv, out):
    q, kz = lv.q, lv.kz

    def along_z(i):
        for j in range(q):
            base = lv.at(i, j, 0)
            flux = [row(lv.f0, lv.edge(i, j))] + [row(lv.fxy, base + 16 * k) for k in range(1, kz)] + [row(lv.fq, lv.edge(i, j))]
            g = lv.diag(flux)
            g = [g[0] + down(g[kz])] + g[1:kz]
            for k in range(kz):
                put(out, base + 16 * k, g[k] + row(lv.mass, base + 16 * k))

    def along_x(j):
        for k in range(kz):
            places = [lv.at(i, j, k) for i in range(q)]
            g = lv.diag([row(lv.fxy, p) for p in places])
            for i in range(q):
                put(out, places[i], row(out, places[i]) + g[i])

    def along_y(i):
        for k in range(kz):
            places = [lv.at(i, j, k) for j in range(q)]
            g = lv.diag([row(lv.fxy, p) for p in places])
            g = [row(out, places[j]) + g[j] for j in range(q)]
            g[0], g[q - 1] = join_y(g[0], g[q - 1])
            for j in range(q):
                put(out, places[j], g[j])

    lv.loop(q, along_z)
    lv.loop(q, along_x)
    lv.loop(q, along_y)
    join_planes_x(lv, out)


DIRS = [(0, 1), (0, -1), (1, 0), (-1, 0), (1, 1), (1, -1), (-1, 1), (-1, -1)]


class Exchange:
    def __init__(self, round_index, fields, offsets, bufs, sems, ids):
        self.r, self.fields, self.ids = round_index, fields, ids
        self.face0, self.corner0 = offsets
        self.face_rows = sum(lv.face for lv, _ in fields)
        self.corner_rows = 8 * len(fields)
        self.bufs, self.sems = bufs, sems
        self.copies = []

    def pack(self):
        sface, scorner = self.bufs[0], self.bufs[2]
        at = self.face0
        for f, (lv, ref) in enumerate(self.fields):
            q, kz = lv.q, lv.kz
            for d, (dx, dy) in enumerate(DIRS[:4]):
                if dy:
                    j, first = (q - 1, 3) if dy > 0 else (0, 0)
                    for i in range(q):
                        for h in range(0, 4 * kz, 8):
                            sface[d, pl.ds(at + i * 4 * kz + h, 8), :] = ref[pl.ds(lv.at(i, j, 0) + first + 4 * h, 8, 4), :]
                else:
                    i = q - 1 if dx > 0 else 0
                    low = lax.broadcasted_iota(jnp.int32, (8, 128), 0) < 4
                    for m in range(0, q * kz, 2):
                        p = lv.at(i, 0, 0) + m * 16
                        if dx > 0:
                            one, two = ref[pl.ds(p + 8, 8), :], ref[pl.ds(p + 24, 8), :]
                            both = jnp.where(low, pltpu.roll(one, 4, 0), two)
                        else:
                            one, two = ref[pl.ds(p, 8), :], ref[pl.ds(p + 16, 8), :]
                            both = jnp.where(low, one, pltpu.roll(two, 4, 0))
                        sface[d, pl.ds(at + m * 4, 8), :] = both
            for c, (dx, dy) in enumerate(DIRS[4:]):
                p = lv.at(q - 1 if dx > 0 else 0, q - 1 if dy > 0 else 0, 0) + (12 if dx > 0 else 0) + (3 if dy > 0 else 0)
                for k in range(kz):
                    scorner[c, pl.ds(self.corner0 + f * 8 + k, 1), :] = ref[pl.ds(p + 16 * k, 1), :]
            at += lv.face

    def send(self):
        sface, rface, scorner, rcorner = self.bufs
        send_sem, recv_sem = self.sems
        x, y, nx, ny = self.ids
        for d, (dx, dy) in enumerate(DIRS):
            if d < 4:
                part = (d, pl.ds(self.face0, self.face_rows), slice(None))
                src, dst = sface.at[part], rface.at[part]
            else:
                part = (d - 4, pl.ds(self.corner0, self.corner_rows), slice(None))
                src, dst = scorner.at[part], rcorner.at[part]
            copy = pltpu.make_async_remote_copy(
                src_ref=src,
                dst_ref=dst,
                send_sem=send_sem.at[self.r, d],
                recv_sem=recv_sem.at[self.r, d],
                device_id=(lax.rem(x + dx + nx, nx), lax.rem(y + dy + ny, ny)),
                device_id_type=MESH,
            )
            copy.start()
            self.copies.append(copy)

    def start(self):
        self.pack()
        self.send()

    def finish(self):
        for copy in self.copies:
            copy.wait_recv()
        rface, rcorner = self.bufs[1], self.bufs[3]
        at = self.face0
        for f, (lv, ref) in enumerate(self.fields):
            q, kz = lv.q, lv.kz
            for d, (dx, dy) in enumerate(DIRS[:4]):
                if dy:
                    j, first = (0, 0) if dy > 0 else (q - 1, 3)
                    for i in range(q):
                        for h in range(0, 4 * kz, 8):
                            place = pl.ds(lv.at(i, j, 0) + first + 4 * h, 8, 4)
                            ref[place, :] = ref[place, :] + rface[d, pl.ds(at + i * 4 * kz + h, 8), :]
                else:
                    i = 0 if dx > 0 else q - 1
                    low = lax.broadcasted_iota(jnp.int32, (8, 128), 0) < 4
                    for m in range(0, q * kz, 2):
                        p = lv.at(i, 0, 0) + m * 16
                        both = rface[d, pl.ds(at + m * 4, 8), :]
                        turned = pltpu.roll(both, 4, 0)
                        if dx > 0:
                            a, b = pl.ds(p, 8), pl.ds(p + 16, 8)
                            ref[a, :] = ref[a, :] + jnp.where(low, both, 0.0)
                            ref[b, :] = ref[b, :] + jnp.where(low, turned, 0.0)
                        else:
                            a, b = pl.ds(p + 8, 8), pl.ds(p + 24, 8)
                            ref[a, :] = ref[a, :] + jnp.where(low, 0.0, turned)
                            ref[b, :] = ref[b, :] + jnp.where(low, 0.0, both)
            for c, (dx, dy) in enumerate(DIRS[4:]):
                p = lv.at(0 if dx > 0 else q - 1, 0 if dy > 0 else q - 1, 0) + (0 if dx > 0 else 12) + (0 if dy > 0 else 3)
                for k in range(kz):
                    place = pl.ds(p + 16 * k, 1)
                    ref[place, :] = ref[place, :] + rcorner[c, pl.ds(self.corner0 + f * 8 + k, 1), :]
            at += lv.face

    def wait_sent(self):
        for copy in self.copies:
            copy.wait_send()


class Lanes:
    def __init__(self, q):
        self.q = q
        step = {k: (k - 128) % q for k in range(q)}
        shift = {0: 0}
        k = 0
        for _ in range(q - 1):
            shift[step[k]] = shift[k] + self.begin(k, 1) - self.begin(step[k], 0)
            k = step[k]
        self.shift = [shift[k] % 128 for k in range(q)]
        lane = lax.broadcasted_iota(jnp.int32, (8, 128), 1)
        self.lane = lane
        self.split_index, self.merge_index = [], []
        for t in range(q):
            place = 128 * t + lane
            k = lax.rem(place, q)
            ez = lax.div(place, q)
            moved = ez
            for node in range(q):
                moved = jnp.where(k == node, ez + self.shift[node], moved)
            self.merge_index.append(jnp.bitwise_and(moved, 127))
            index = jnp.zeros((8, 128), jnp.int32)
            for node in range(q):
                ez = jnp.bitwise_and(lane - self.shift[node] + 128, 127)
                index = jnp.where(self.inside(node, t), q * ez + node - 128 * t, index)
            self.split_index.append(index)

    def begin(self, k, t):
        return -((k - 128 * t) // self.q)

    def inside(self, k, t):
        lo, hi = (self.begin(k, t) + self.shift[k]) % 128, (self.begin(k, t + 1) + self.shift[k]) % 128
        if lo < hi:
            return (self.lane >= lo) & (self.lane < hi) if lo else self.lane < hi
        return (self.lane >= lo) | (self.lane < hi) if hi else self.lane >= lo

    @staticmethod
    def gather(x, index):
        numbers = lax.GatherDimensionNumbers(
            offset_dims=(), collapsed_slice_dims=(1,), start_index_map=(1,), operand_batching_dims=(0,), start_indices_batching_dims=(0,)
        )
        return lax.gather(x, index[..., None], numbers, slice_sizes=(1, 1), mode=lax.GatherScatterMode.PROMISE_IN_BOUNDS)

    def split(self, stored):
        moved = [self.gather(stored[t], self.split_index[t]) for t in range(self.q)]
        out = []
        for k in range(self.q):
            x = moved[0]
            for t in range(1, self.q):
                x = jnp.where(self.inside(k, t), moved[t], x)
            out.append(pltpu.roll(x, (128 - self.shift[k]) % 128, 1) if self.shift[k] else x)
        return out

    def merge(self, nodes):
        moved = [pltpu.roll(nodes[k], self.shift[k], 1) if self.shift[k] else nodes[k] for k in range(self.q)]
        out = []
        for t in range(self.q):
            x = moved[0]
            for k in range(1, self.q):
                x = jnp.where(self.inside(k, t), moved[k], x)
            out.append(self.gather(x, self.merge_index[t]))
        return out


def pick(i, values):
    out = jnp.asarray(values[-1], F32)
    for n in range(len(values) - 2, -1, -1):
        out = jnp.where(i == n, jnp.asarray(values[n], F32), out)
    return out


def load_field(lanes, raw, store):
    def body(i):
        wx = pick(i, WF)
        for j in range(5):
            halves = []
            for h in range(2):
                stored = []
                for t in range(5):
                    low = raw[t, 10 * h + i, pl.ds(j, 4, 5), :]
                    high = raw[t, 10 * h + 5 + i, pl.ds(j, 4, 5), :]
                    stored.append(jnp.concatenate([low, high], axis=0))
                halves.append(lanes.split(stored))
            planes = [jnp.concatenate([halves[0][k], halves[1][k]], axis=0) * (wx * (WF[j] * WF[k])) for k in range(5)]
            store(i, j, planes)

    loop(5, body)


FR, CR, ER, CER = 1600, 288, 400, 144


def cheb_weights():
    sigma, rho = 5.0 / 3.0, 0.6
    theta, delta = 0.75, 0.45
    d = np.array([1.0 / theta, 0.0, 0.0])
    x = np.zeros(3)
    for sweep in range(SWEEPS):
        x = x + d
        if sweep + 1 < SWEEPS:
            nxt = 1.0 / (2.0 * sigma - rho)
            res = np.array([1.0, 0.0, 0.0]) - np.concatenate([[0.0], x[:-1]])
            d = nxt * rho * d + 2.0 * nxt / delta * res
            rho = nxt
    return [float(c) for c in x]


CHEB = cheb_weights()

ROUNDS = [(1, 1), (1, 1), (1, 1), (1, 1), (1, 1), (1, 1), (0, 1), (0, 1), (0, 1)]


def round_offsets():
    face, corner, out = 0, 0, []
    for fine, coarse in ROUNDS:
        out.append((face, corner))
        face += 80 * fine + 24 * coarse
        corner += 8 * (fine + coarse)
    return out, face, corner


OFFSETS, FACE_ROWS, CORNER_ROWS = round_offsets()


def kernel(nx, ny, src, cond, absn, out_ref, corr_ref, *s):
    (raw, obuf, cbuf, fxy, f0, f4, mass, inv, load, u0, u1, u2, pa, first, pb, ca, cb, last, tmp,
     cfxy, cf0, cf2, cmass, cinv, rl, cfirst, qa, qb, ra0, ra1, ra2, w0, w1, wa, wb, corr,
     s1, s2, s3, s4, ar1, ar2, arx, ary, sface, rface, scorner, rcorner,
     in_sem, out_sem, cout_sem, send_sem, recv_sem, ax_send, ax_recv, ay_send, ay_recv) = s
    x, y = lax.axis_index("gx"), lax.axis_index("gy")

    inputs = []
    for a, ref in enumerate((cond, absn, src)):
        for t in range(5):
            copy = pltpu.make_async_copy(ref.at[:, :, pl.ds(128 * t, 128)], raw.at[a, t], in_sem.at[a, t])
            copy.start()
            inputs.append(copy)

    def x_peer(d):
        return (lax.rem(x + d + nx, nx), y)

    def y_peer(d):
        return (x, lax.rem(y + d + ny, ny))

    barrier = pltpu.get_barrier_semaphore()
    greeted = [(lax.rem(x + dx + nx, nx), lax.rem(y + dy + ny, ny)) for dx, dy in DIRS[4:]]
    greeted += [x_peer(d) for d in range(1, nx)] + [y_peer(d) for d in range(1, ny)]
    for peer in greeted:
        pl.semaphore_signal(barrier, inc=1, device_id=peer, device_id_type=MESH)

    lf = Level(5, fxy, f0, f4, mass, inv)
    lc = Level(3, cfxy, cf0, cf2, cmass, cinv)
    bufs, sems, ids = (sface, rface, scorner, rcorner), (send_sem, recv_sem), (x, y, nx, ny)
    rounds = []

    def exchange(index, *fields):
        assert ROUNDS[index] == (sum(lv.q == 5 for lv, _ in fields), sum(lv.q == 3 for lv, _ in fields))
        e = Exchange(index, fields, OFFSETS[index], bufs, sems, ids)
        rounds.append(e)
        e.start()
        return e

    lanes = Lanes(5)

    def store_flux(i, j, p):
        put(f0, lf.edge(i, j), p[0])
        put(f4, lf.edge(i, j), p[4])
        put(fxy, lf.at(i, j, 0), p[0] + down(p[4]))
        for k in range(1, 4):
            put(fxy, lf.at(i, j, k), p[k])

    def store_plain(ref):
        def store(i, j, p):
            put(ref, lf.at(i, j, 0), p[0] + down(p[4]))
            for k in range(1, 4):
                put(ref, lf.at(i, j, k), p[k])

        return store

    for copy in inputs[:5]:
        copy.wait()
    load_field(lanes, raw.at[0], store_flux)
    for copy in inputs[5:10]:
        copy.wait()
    load_field(lanes, raw.at[1], store_plain(mass))
    for i in range(3):
        for j in range(3):
            ratio = WC[i] * WC[j] / (WF[2 * i] * WF[2 * j])
            ends, mid = ratio * WC[0] / WF[0], ratio * WC[1] / WF[2]
            put(cf0, lc.edge(i, j), ends * row(f0, lf.edge(2 * i, 2 * j)))
            put(cf2, lc.edge(i, j), ends * row(f4, lf.edge(2 * i, 2 * j)))
            for a, b in ((cfxy, fxy), (cmass, mass)):
                put(a, lc.at(i, j, 0), ends * row(b, lf.at(2 * i, 2 * j, 0)))
                put(a, lc.at(i, j, 1), mid * row(b, lf.at(2 * i, 2 * j, 2)))
    local_diag(lf, inv)
    local_diag(lc, cinv)

    pl.semaphore_wait(barrier, len(greeted))
    e_diag = exchange(0, (lf, inv), (lc, cinv))

    for copy in inputs[10:]:
        copy.wait()
    load_field(lanes, raw.at[2], store_plain(load))
    restrict_y(lf, load, tmp)
    join_planes_y(lf, load)
    join_planes_x(lf, load)
    restrict_xz(lc, tmp, rl)
    e_load = exchange(1, (lf, load), (lc, rl))

    def invert(lv):
        def body(i):
            for n in range(lv.q * lv.kz):
                p = lv.at(i, 0, 0) + n * 16
                put(lv.inv, p, 1.0 / row(lv.inv, p))

        lv.loop(lv.q, body)

    e_diag.finish()
    invert(lf)
    invert(lc)
    e_load.finish()

    apply_local(lf, pa, load)
    apply_local(lc, qa, rl)
    e_pa = exchange(2, (lf, pa), (lc, qa))
    apply_local(lf, ca, u0, scaled=load, restrict=tmp)
    restrict_xz(lc, tmp, ra0)
    e_ca = exchange(3, (lf, ca), (lc, ra0))
    e_pa.finish()
    apply_local(lf, pb, first, scaled=pa, sums=s1)
    apply_local(lc, qb, cfirst, scaled=qa, sums=s3)
    e_pb = exchange(4, (lf, pb), (lc, qb))
    e_ca.finish()
    apply_local(lf, cb, u1, scaled=ca, restrict=tmp)
    restrict_xz(lc, tmp, ra1)
    e_cb = exchange(5, (lf, cb), (lc, ra1))
    e_pb.finish()
    sum_squares(lf, pb, s2)
    sum_squares(lc, qb, s4)

    def fold(sums):
        return jnp.sum(sums[...], axis=0, keepdims=True)

    def to_all(source, slots, count, peer, send, recv):
        copies = []
        for d in range(1, count):
            copy = pltpu.make_async_remote_copy(
                src_ref=source, dst_ref=slots.at[d], send_sem=send.at[d], recv_sem=recv.at[d], device_id=peer(d), device_id_type=MESH
            )
            copy.start()
            copies.append(copy)
        return copies

    def gathered(source, slots, count, copies):
        for copy in copies:
            copy.wait_recv()
        total = source[...]
        for d in range(1, count):
            total = total + slots[d]
        return total

    ar1[...] = jnp.concatenate([fold(s1), fold(s2), fold(s3), fold(s4), jnp.zeros((4, 128), F32)], axis=0)
    x_copies = to_all(ar1, arx, nx, x_peer, ax_send, ax_recv)

    e_cb.finish()
    apply_local(lf, last, u2, scaled=cb, restrict=tmp, keep=False)
    restrict_xz(lc, tmp, ra2)
    e_ra2 = exchange(6, (lc, ra2))

    ar2[...] = gathered(ar1, arx, nx, x_copies)
    y_copies = to_all(ar2, ary, ny, y_peer, ay_send, ay_recv)
    e_ra2.finish()
    totals = jnp.sum(gathered(ar2, ary, ny, y_copies), axis=1, keepdims=True)

    def inverse_estimate(n):
        estimate = jnp.sqrt(totals[n + 1 : n + 2] / (totals[n : n + 1] + 1e-06))
        return jnp.broadcast_to(1.0 / estimate, (16, 128))

    g, gc = inverse_estimate(0), inverse_estimate(2)

    def horner(scale, a, b, c):
        return scale * (CHEB[0] * a + scale * (CHEB[1] * b + scale * (CHEB[2] * c)))

    for n in range(18):
        p = 16 * n
        put(wa, p, row(rl, p) - horner(g, row(ra0, p), row(ra1, p), row(ra2, p)))
    apply_local(lc, wb, w0, scaled=wa)
    e_w0 = exchange(7, (lc, wb))

    def smooth(i):
        for n in range(20):
            p = lf.at(i, 0, 0) + 16 * n
            put(u0, p, horner(g, row(u0, p), row(u1, p), row(u2, p)))

    loop(5, smooth)
    e_w0.finish()
    apply_local(lc, last, w1, scaled=wb)
    e_w1 = exchange(8, (lc, last))
    e_w1.finish()

    pieces3 = Lanes(3)
    copies = []
    for i in range(3):
        for j in range(3):
            for k in range(2):
                p = lc.at(i, j, k)
                w2 = row(last, p) * row(cinv, p)
                put(corr, p, horner(gc, row(w0, p), row(w1, p), w2))
            c = [row(corr, lc.at(i, j, 0)), row(corr, lc.at(i, j, 1))]
            c.append(up(c[0]))
            for h in range(2):
                stored = pieces3.merge([v[8 * h : 8 * h + 8] for v in c])
                for t in range(3):
                    cbuf[t, 6 * h + i, pl.ds(j, 4, 3), :] = stored[t][:4]
                    cbuf[t, 6 * h + 3 + i, pl.ds(j, 4, 3), :] = stored[t][4:]
    for t in range(3):
        copy = pltpu.make_async_copy(cbuf.at[t], corr_ref.at[:, :, pl.ds(128 * t, 128)], cout_sem.at[t])
        copy.start()
        copies.append(copy)

    for i in range(3):
        lines = []
        for j in range(3):
            a, b = row(corr, lc.at(i, j, 0)), row(corr, lc.at(i, j, 1))
            c = up(a)
            lines.append([a, JA * a + JB * b + JC * c, b, JC * a + JB * b + JA * c])
        for k in range(4):
            a, b, c = lines[0][k], lines[1][k], lines[2][k]
            for j, v in enumerate([a, JA * a + JB * b + JC * c, b, JC * a + JB * b + JA * c, c]):
                put(tmp, ((i * 5 + j) * 4 + k) * 16, v)

    def finish_plane(i):
        cx = [pick(i, [r[c] for r in JROWS]) for c in range(3)]
        for j in range(5):
            planes = []
            for k in range(4):
                lifted = [row(tmp, ((c * 5 + j) * 4 + k) * 16) for c in range(3)]
                lifted = cx[0] * lifted[0] + cx[1] * lifted[1] + cx[2] * lifted[2]
                planes.append(row(u0, lf.at(i, j, k)) + lifted)
            planes.append(up(planes[0]))
            for h in range(2):
                stored = lanes.merge([v[8 * h : 8 * h + 8] for v in planes])
                for t in range(5):
                    obuf[t, 10 * h + i, pl.ds(j, 4, 5), :] = stored[t][:4]
                    obuf[t, 10 * h + 5 + i, pl.ds(j, 4, 5), :] = stored[t][4:]

    loop(5, finish_plane)
    for t in range(5):
        copy = pltpu.make_async_copy(obuf.at[t], out_ref.at[:, :, pl.ds(128 * t, 128)], out_sem.at[t])
        copy.start()
        copies.append(copy)
    for e in rounds:
        e.wait_sent()
    for copy in x_copies + y_copies:
        copy.wait_send()
    for copy in copies:
        copy.wait()


def scratch(nx, ny):
    def v(*shape):
        return pltpu.VMEM(shape, F32)

    fine, coarse = v(FR, 128), v(CR, 128)
    dma = pltpu.SemaphoreType.DMA
    return (
        [v(3, 5, 20, 20, 128), v(5, 20, 20, 128), v(3, 12, 12, 128)]
        + [fine, v(ER, 128), v(ER, 128)]
        + [fine] * 12
        + [v(960, 128)]
        + [coarse, v(CER, 128), v(CER, 128)]
        + [coarse] * 14
        + [v(16, 128)] * 4
        + [v(8, 128), v(8, 128), v(nx, 8, 128), v(ny, 8, 128)]
        + [v(4, FACE_ROWS, 128)] * 2
        + [v(4, CORNER_ROWS, 128)] * 2
        + [dma((3, 5)), dma((5,)), dma((3,)), dma((len(ROUNDS), 8)), dma((len(ROUNDS), 8))]
        + [dma((nx,)), dma((nx,)), dma((ny,)), dma((ny,))]
    )


def solution(mesh):
    nx, ny = mesh.shape["gx"], mesh.shape["gy"]

    def on_device(source, conductivity, absorption):
        return pl.pallas_call(
            functools.partial(kernel, nx, ny),
            out_shape=(jax.ShapeDtypeStruct((20, 20, 640), F32), jax.ShapeDtypeStruct((12, 12, 384), F32)),
            in_specs=[pl.BlockSpec(memory_space=pl.ANY)] * 3,
            out_specs=[pl.BlockSpec(memory_space=pl.ANY)] * 2,
            scratch_shapes=scratch(nx, ny),
            compiler_params=pltpu.CompilerParams(collective_id=0, has_side_effects=True, vmem_limit_bytes=60 * 1024 * 1024),
            name="window",
        )(source, conductivity, absorption)

    placed = P("gx", "gy", None)
    return jax.shard_map(on_device, mesh=mesh, in_specs=(placed,) * 3, out_specs=(placed, placed), check_vma=False)
```

```python
import functools
import math

import jax
import jax.numpy as jnp
import numpy as np
from jax import lax
from jax.experimental import pallas as pl
from jax.experimental.pallas import tpu as pltpu
from jax.sharding import PartitionSpec as P

MESH = pl.DeviceIdType.MESH
SWEEPS = 3
F32 = jnp.float32


def deriv_table(points):
    count = len(points)
    bary = [1.0 / np.prod([points[j] - points[k] for k in range(count) if k != j]) for j in range(count)]
    table = np.zeros((count, count))
    for i in range(count):
        for j in range(count):
            if i != j:
                table[i, j] = bary[j] / (bary[i] * (points[i] - points[j]))
        table[i, i] = -np.sum(table[i])
    return table


ROOT = math.sqrt(3.0 / 7.0)
WF = [0.1, 49.0 / 90.0, 32.0 / 45.0, 49.0 / 90.0, 0.1]
WC = [1.0 / 3.0, 4.0 / 3.0, 1.0 / 3.0]
DF = deriv_table(np.array([-1.0, -ROOT, 0.0, ROOT, 1.0]))
JA, JB, JC = (ROOT * ROOT + ROOT) / 2, 1 - ROOT * ROOT, (ROOT * ROOT - ROOT) / 2
JROWS = [[1.0, 0.0, 0.0], [JA, JB, JC], [0.0, 1.0, 0.0], [JC, JB, JA], [0.0, 0.0, 1.0]]


B00, B01 = (DF[4][4] + DF[0][4]) / 2, (DF[4][3] + DF[0][3]) / 2
B10, B11 = (DF[3][4] + DF[1][4]) / 2, (DF[3][3] + DF[1][3]) / 2
G00, G01 = (DF[4][4] - DF[0][4]) / 2, (DF[4][3] - DF[0][3]) / 2
G10, G11 = (DF[3][4] - DF[1][4]) / 2, (DF[3][3] - DF[1][3]) / 2
A0, A1 = DF[2][4], DF[2][3]


def stiff5(v, flux):
    a0, a1 = v[4] - v[0], v[3] - v[1]
    m2 = v[2] + v[2]
    s0, s1 = v[0] + v[4] - m2, v[1] + v[3] - m2
    p0, p1 = B00 * a0 + B01 * a1, B10 * a0 + B11 * a1
    q0, q1 = G00 * s0 + G01 * s1, G10 * s0 + G11 * s1
    f0, f4 = flux[0] * (p0 - q0), flux[4] * (p0 + q0)
    f1, f3 = flux[1] * (p1 - q1), flux[3] * (p1 + q1)
    f2 = flux[2] * (A0 * a0 + A1 * a1)
    sp0, sq0, sp1, sq1 = f4 + f0, f4 - f0, f3 + f1, f3 - f1
    b0 = A0 * f2 + B00 * sp0 + B10 * sp1
    b1 = A1 * f2 + B01 * sp0 + B11 * sp1
    c0, c1 = G00 * sq0 + G10 * sq1, G01 * sq0 + G11 * sq1
    mid = c0 + c1
    return [c0 - b0, c1 - b1, -(mid + mid), c1 + b1, c0 + b0]


DD = (DF * DF).T


def diag5(flux):
    s0, s1, d0, d1 = flux[0] + flux[4], flux[1] + flux[3], flux[0] - flux[4], flux[1] - flux[3]
    out = [None] * 5
    for r in (0, 1):
        even = (DD[r][0] + DD[r][4]) / 2 * s0 + (DD[r][1] + DD[r][3]) / 2 * s1 + DD[r][2] * flux[2]
        odd = (DD[r][0] - DD[r][4]) / 2 * d0 + (DD[r][1] - DD[r][3]) / 2 * d1
        out[r], out[4 - r] = even + odd, even - odd
    out[2] = DD[2][0] * s0 + DD[2][1] * s1
    return out


def stiff3(v, flux):
    a = 0.5 * (v[2] - v[0])
    s = v[0] + v[2] - (v[1] + v[1])
    f0, f1, f2 = flux[0] * (a - s), flux[1] * a, flux[2] * (a + s)
    b = 0.5 * (f0 + f1 + f2)
    t = f2 - f0
    return [t - b, -(t + t), t + b]


DC = deriv_table(np.array([-1.0, 0.0, 1.0]))
DDC = (DC * DC).T


def diag3(flux):
    s = flux[0] + flux[2]
    return [
        DDC[0][0] * flux[0] + DDC[0][1] * flux[1] + DDC[0][2] * flux[2],
        DDC[1][0] * s,
        DDC[2][0] * flux[0] + DDC[2][1] * flux[1] + DDC[2][2] * flux[2],
    ]


def restrict5(y):
    return [y[0] + JA * y[1] + JC * y[3], JB * (y[1] + y[3]) + y[2], y[4] + JC * y[1] + JA * y[3]]


def up(x):
    return pltpu.roll(x, 127, 1)


def down(x):
    return pltpu.roll(x, 1, 1)


def loop(count, body):
    def step(i, carry):
        body(i)
        return carry

    lax.fori_loop(0, count, step, 0)


def unrolled(count, body):
    for i in range(count):
        body(i)


class Level:
    def __init__(self, q, fxy, f0, fq, mass, inv):
        self.q, self.kz = q, q - 1
        self.fxy, self.f0, self.fq, self.mass, self.inv = fxy, f0, fq, mass, inv
        self.stiff, self.diag = (stiff5, diag5) if q == 5 else (stiff3, diag3)
        self.face = q * self.kz * 4

    def at(self, i, j, k):
        return ((i * self.q + j) * self.kz + k) * 16

    def edge(self, i, j):
        return (i * self.q + j) * 16


def row(ref, start):
    if not isinstance(start, int):
        start = pl.multiple_of(start, 16)
    return ref[pl.ds(start, 16), :]


def put(ref, start, value):
    if not isinstance(start, int):
        start = pl.multiple_of(start, 16)
    ref[pl.ds(start, 16), :] = value


def element_rows():
    e = lax.broadcasted_iota(jnp.int32, (16, 128), 0)
    return e // 4, e % 4


def join_y(lo, hi):
    _, ey = element_rows()
    hi = hi + jnp.where(ey < 3, pltpu.roll(lo, 15, 0), 0.0)
    return jnp.where(ey > 0, pltpu.roll(hi, 1, 0), lo), hi


def join_x(lo, hi):
    ex, _ = element_rows()
    hi = hi + jnp.where(ex < 3, pltpu.roll(lo, 12, 0), 0.0)
    return jnp.where(ex > 0, pltpu.roll(hi, 4, 0), lo), hi


def join_planes_x(lv, out):
    q, kz = lv.q, lv.kz

    def body(j):
        for k in range(kz):
            lo, hi = join_x(row(out, lv.at(0, j, k)), row(out, lv.at(q - 1, j, k)))
            put(out, lv.at(0, j, k), lo)
            put(out, lv.at(q - 1, j, k), hi)

    unrolled(q, body)


def join_planes_y(lv, out):
    q, kz = lv.q, lv.kz

    def body(i):
        for k in range(kz):
            lo, hi = join_y(row(out, lv.at(i, 0, k)), row(out, lv.at(i, q - 1, k)))
            put(out, lv.at(i, 0, k), lo)
            put(out, lv.at(i, q - 1, k), hi)

    unrolled(q, body)


def apply_local(lv, out, u, scaled=None, sums=None, restrict=None, keep=True):
    q, kz = lv.q, lv.kz

    def along_z(i):
        total = None
        for j in range(q):
            base = lv.at(i, j, 0)
            if scaled is None:
                v = [row(u, base + 16 * k) for k in range(kz)]
            else:
                v = [row(scaled, base + 16 * k) * row(lv.inv, base + 16 * k) for k in range(kz)]
                for k in range(kz):
                    put(u, base + 16 * k, v[k])
                if sums is not None:
                    part = v[0] * v[0]
                    part = part + part
                    for k in range(1, kz):
                        part = part + v[k] * v[k]
                    total = part if total is None else total + part
            flux = [row(lv.f0, lv.edge(i, j))] + [row(lv.fxy, base + 16 * k) for k in range(1, kz)] + [row(lv.fq, lv.edge(i, j))]
            g = lv.stiff(v + [up(v[0])], flux)
            g = [g[0] + down(g[kz])] + g[1:kz]
            for k in range(kz):
                put(out, base + 16 * k, g[k] + row(lv.mass, base + 16 * k) * v[k])
        if sums is not None:
            sums[...] += total

    def along_x(j):
        for k in range(kz):
            places = [lv.at(i, j, k) for i in range(q)]
            g = lv.stiff([row(u, p) for p in places], [row(lv.fxy, p) for p in places])
            for i in range(q):
                put(out, places[i], row(out, places[i]) + g[i])

    def along_y(i):
        for k in range(kz):
            places = [lv.at(i, j, k) for j in range(q)]
            g = lv.stiff([row(u, p) for p in places], [row(lv.fxy, p) for p in places])
            g = [row(out, places[j]) + g[j] for j in range(q)]
            if restrict is not None:
                c = restrict5(g)
                for jc in range(3):
                    put(restrict, ((i * 3 + jc) * 4 + k) * 16, c[jc])
            if keep:
                g[0], g[q - 1] = join_y(g[0], g[q - 1])
                for j in range(q):
                    put(out, places[j], g[j])

    if sums is not None:
        sums[...] = jnp.zeros_like(sums)
    unrolled(q, along_z)
    unrolled(q, along_x)
    unrolled(q, along_y)
    if keep:
        join_planes_x(lv, out)


def sum_squares(lv, scaled, sums):
    total = [None] * 4
    for i in range(lv.q - 1):
        for j in range(lv.q - 1):
            for k in range(lv.kz):
                p = lv.at(i, j, k)
                v = row(scaled, p) * row(lv.inv, p)
                v = v * v
                zeros = (i == 0) + (j == 0) + (k == 0)
                total[zeros] = v if total[zeros] is None else total[zeros] + v
    sums[...] = total[0] + 2.0 * total[1] + 4.0 * total[2] + 8.0 * total[3]


def restrict_xz(lc, tmp, out):
    for jc in range(3):
        cols = [restrict5([row(tmp, ((i * 3 + jc) * 4 + k) * 16) for i in range(5)]) for k in range(4)]
        for ic in range(3):
            y = [cols[k][ic] for k in range(4)]
            first = y[0] + JA * y[1] + JC * y[3] + down(JC * y[1] + JA * y[3])
            put(out, lc.at(ic, jc, 0), first)
            put(out, lc.at(ic, jc, 1), JB * (y[1] + y[3]) + y[2])
    join_planes_y(lc, out)
    join_planes_x(lc, out)


def restrict_y(lv, src, tmp):
    def body(i):
        for k in range(4):
            c = restrict5([row(src, lv.at(i, j, k)) for j in range(5)])
            for jc in range(3):
                put(tmp, ((i * 3 + jc) * 4 + k) * 16, c[jc])

    unrolled(5, body)


def local_diag(lv, out):
    q, kz = lv.q, lv.kz

    def along_z(i):
        for j in range(q):
            base = lv.at(i, j, 0)
            flux = [row(lv.f0, lv.edge(i, j))] + [row(lv.fxy, base + 16 * k) for k in range(1, kz)] + [row(lv.fq, lv.edge(i, j))]
            g = lv.diag(flux)
            g = [g[0] + down(g[kz])] + g[1:kz]
            for k in range(kz):
                put(out, base + 16 * k, g[k] + row(lv.mass, base + 16 * k))

    def along_x(j):
        for k in range(kz):
            places = [lv.at(i, j, k) for i in range(q)]
            g = lv.diag([row(lv.fxy, p) for p in places])
            for i in range(q):
                put(out, places[i], row(out, places[i]) + g[i])

    def along_y(i):
        for k in range(kz):
            places = [lv.at(i, j, k) for j in range(q)]
            g = lv.diag([row(lv.fxy, p) for p in places])
            g = [row(out, places[j]) + g[j] for j in range(q)]
            g[0], g[q - 1] = join_y(g[0], g[q - 1])
            for j in range(q):
                put(out, places[j], g[j])

    unrolled(q, along_z)
    unrolled(q, along_x)
    unrolled(q, along_y)
    join_planes_x(lv, out)


DIRS = [(0, 1), (0, -1), (1, 0), (-1, 0), (1, 1), (1, -1), (-1, 1), (-1, -1)]


class Exchange:
    def __init__(self, round_index, fields, offsets, bufs, sems, ids, forward):
        self.r, self.fields, self.ids = round_index, fields, ids
        self.face0, self.corner0 = offsets
        self.face_rows = sum(lv.face for lv, _ in fields)
        self.corner_rows = 8 * len(fields)
        self.bufs, self.sems = bufs, sems
        self.dirs = [d for d, (dx, dy) in enumerate(DIRS) if not forward or (dx >= 0 and dy >= 0)]
        self.copies = []

    def pack(self):
        sface, scorner = self.bufs[0], self.bufs[2]
        at = self.face0
        for f, (lv, ref) in enumerate(self.fields):
            q, kz = lv.q, lv.kz
            for d, (dx, dy) in enumerate(DIRS[:4]):
                if d not in self.dirs:
                    continue
                if dy:
                    j, first = (q - 1, 3) if dy > 0 else (0, 0)
                    for i in range(q):
                        for h in range(0, 4 * kz, 8):
                            sface[d, pl.ds(at + i * 4 * kz + h, 8), :] = ref[pl.ds(lv.at(i, j, 0) + first + 4 * h, 8, 4), :]
                else:
                    i = q - 1 if dx > 0 else 0
                    low = lax.broadcasted_iota(jnp.int32, (8, 128), 0) < 4
                    for m in range(0, q * kz, 2):
                        p = lv.at(i, 0, 0) + m * 16
                        if dx > 0:
                            one, two = ref[pl.ds(p + 8, 8), :], ref[pl.ds(p + 24, 8), :]
                            both = jnp.where(low, pltpu.roll(one, 4, 0), two)
                        else:
                            one, two = ref[pl.ds(p, 8), :], ref[pl.ds(p + 16, 8), :]
                            both = jnp.where(low, one, pltpu.roll(two, 4, 0))
                        sface[d, pl.ds(at + m * 4, 8), :] = both
            for c, (dx, dy) in enumerate(DIRS[4:]):
                if c + 4 not in self.dirs:
                    continue
                p = lv.at(q - 1 if dx > 0 else 0, q - 1 if dy > 0 else 0, 0) + (12 if dx > 0 else 0) + (3 if dy > 0 else 0)
                for k in range(kz):
                    scorner[c, pl.ds(self.corner0 + f * 8 + k, 1), :] = ref[pl.ds(p + 16 * k, 1), :]
            at += lv.face

    def send(self):
        sface, rface, scorner, rcorner = self.bufs
        send_sem, recv_sem = self.sems
        x, y, nx, ny = self.ids
        for d in self.dirs:
            dx, dy = DIRS[d]
            if d < 4:
                part = (d, pl.ds(self.face0, self.face_rows), slice(None))
                src, dst = sface.at[part], rface.at[part]
            else:
                part = (d - 4, pl.ds(self.corner0, self.corner_rows), slice(None))
                src, dst = scorner.at[part], rcorner.at[part]
            copy = pltpu.make_async_remote_copy(
                src_ref=src,
                dst_ref=dst,
                send_sem=send_sem.at[self.r, d],
                recv_sem=recv_sem.at[self.r, d],
                device_id=(lax.rem(x + dx + nx, nx), lax.rem(y + dy + ny, ny)),
                device_id_type=MESH,
            )
            copy.start()
            self.copies.append(copy)

    def start(self):
        self.pack()
        self.send()

    def finish(self):
        for copy in self.copies:
            copy.wait_recv()
        rface, rcorner = self.bufs[1], self.bufs[3]
        at = self.face0
        for f, (lv, ref) in enumerate(self.fields):
            q, kz = lv.q, lv.kz
            for d, (dx, dy) in enumerate(DIRS[:4]):
                if d not in self.dirs:
                    continue
                if dy:
                    j, first = (0, 0) if dy > 0 else (q - 1, 3)
                    for i in range(q):
                        for h in range(0, 4 * kz, 8):
                            place = pl.ds(lv.at(i, j, 0) + first + 4 * h, 8, 4)
                            ref[place, :] = ref[place, :] + rface[d, pl.ds(at + i * 4 * kz + h, 8), :]
                else:
                    i = 0 if dx > 0 else q - 1
                    low = lax.broadcasted_iota(jnp.int32, (8, 128), 0) < 4
                    for m in range(0, q * kz, 2):
                        p = lv.at(i, 0, 0) + m * 16
                        both = rface[d, pl.ds(at + m * 4, 8), :]
                        turned = pltpu.roll(both, 4, 0)
                        if dx > 0:
                            a, b = pl.ds(p, 8), pl.ds(p + 16, 8)
                            ref[a, :] = ref[a, :] + jnp.where(low, both, 0.0)
                            ref[b, :] = ref[b, :] + jnp.where(low, turned, 0.0)
                        else:
                            a, b = pl.ds(p + 8, 8), pl.ds(p + 24, 8)
                            ref[a, :] = ref[a, :] + jnp.where(low, 0.0, turned)
                            ref[b, :] = ref[b, :] + jnp.where(low, 0.0, both)
            for c, (dx, dy) in enumerate(DIRS[4:]):
                if c + 4 not in self.dirs:
                    continue
                p = lv.at(0 if dx > 0 else q - 1, 0 if dy > 0 else q - 1, 0) + (0 if dx > 0 else 12) + (0 if dy > 0 else 3)
                for k in range(kz):
                    place = pl.ds(p + 16 * k, 1)
                    ref[place, :] = ref[place, :] + rcorner[c, pl.ds(self.corner0 + f * 8 + k, 1), :]
            at += lv.face

    def wait_sent(self):
        for copy in self.copies:
            copy.wait_send()


class Lanes:
    def __init__(self, q):
        self.q = q
        step = {k: (k - 128) % q for k in range(q)}
        shift = {0: 0}
        k = 0
        for _ in range(q - 1):
            shift[step[k]] = shift[k] + self.begin(k, 1) - self.begin(step[k], 0)
            k = step[k]
        self.shift = [shift[k] % 128 for k in range(q)]
        lane = lax.broadcasted_iota(jnp.int32, (8, 128), 1)
        self.lane = lane
        self.split_index, self.merge_index = [], []
        for t in range(q):
            place = 128 * t + lane
            k = lax.rem(place, q)
            ez = lax.div(place, q)
            moved = ez
            for node in range(q):
                moved = jnp.where(k == node, ez + self.shift[node], moved)
            self.merge_index.append(jnp.bitwise_and(moved, 127))
            index = jnp.zeros((8, 128), jnp.int32)
            for node in range(q):
                ez = jnp.bitwise_and(lane - self.shift[node] + 128, 127)
                index = jnp.where(self.inside(node, t), q * ez + node - 128 * t, index)
            self.split_index.append(index)

    def begin(self, k, t):
        return -((k - 128 * t) // self.q)

    def inside(self, k, t):
        lo, hi = (self.begin(k, t) + self.shift[k]) % 128, (self.begin(k, t + 1) + self.shift[k]) % 128
        if lo < hi:
            return (self.lane >= lo) & (self.lane < hi) if lo else self.lane < hi
        return (self.lane >= lo) | (self.lane < hi) if hi else self.lane >= lo

    @staticmethod
    def gather(x, index):
        numbers = lax.GatherDimensionNumbers(
            offset_dims=(), collapsed_slice_dims=(1,), start_index_map=(1,), operand_batching_dims=(0,), start_indices_batching_dims=(0,)
        )
        return lax.gather(x, index[..., None], numbers, slice_sizes=(1, 1), mode=lax.GatherScatterMode.PROMISE_IN_BOUNDS)

    def unmix(self, moved):
        out = []
        for k in range(self.q):
            x = moved[0]
            for t in range(1, self.q):
                x = jnp.where(self.inside(k, t), moved[t], x)
            out.append(pltpu.roll(x, (128 - self.shift[k]) % 128, 1) if self.shift[k] else x)
        return out

    def mix(self, nodes):
        moved = [pltpu.roll(nodes[k], self.shift[k], 1) if self.shift[k] else nodes[k] for k in range(self.q)]
        out = []
        for t in range(self.q):
            x = moved[0]
            for k in range(1, self.q):
                x = jnp.where(self.inside(k, t), moved[k], x)
            out.append(x)
        return out


def pick(i, values):
    out = jnp.asarray(values[-1], F32)
    for n in range(len(values) - 2, -1, -1):
        out = jnp.where(i == n, jnp.asarray(values[n], F32), out)
    return out


def load_field(lanes, ref, raw, index, buf, sem, store):
    def tile(t):
        pltpu.make_async_copy(ref.at[:, :, pl.ds(pl.multiple_of(128 * t, 128), 128)], raw.at[t], sem.at[t]).wait()
        order = index[t]
        for i in range(5):
            for j in range(5):
                for h in range(2):
                    low = raw[t, 10 * h + i, pl.ds(j, 4, 5), :]
                    high = raw[t, 10 * h + 5 + i, pl.ds(j, 4, 5), :]
                    both = jnp.concatenate([low, high], axis=0)
                    buf[t, pl.ds((i * 5 + j) * 16 + 8 * h, 8), :] = lanes.gather(both, order)

    def plane(i):
        wx = pick(i, WF)
        for j in range(5):
            halves = []
            for h in range(2):
                p = pl.ds(pl.multiple_of((i * 5 + j) * 16 + 8 * h, 8), 8)
                halves.append(lanes.unmix([buf[t, p, :] for t in range(5)]))
            store(i, j, [jnp.concatenate([halves[0][k], halves[1][k]], axis=0) * (wx * (WF[j] * WF[k])) for k in range(5)])

    loop(5, tile)
    loop(5, plane)


FR, CR, ER, CER = 1600, 288, 400, 144


def cheb_weights():
    sigma, rho = 5.0 / 3.0, 0.6
    theta, delta = 0.75, 0.45
    d = np.array([1.0 / theta, 0.0, 0.0])
    x = np.zeros(3)
    for sweep in range(SWEEPS):
        x = x + d
        if sweep + 1 < SWEEPS:
            nxt = 1.0 / (2.0 * sigma - rho)
            res = np.array([1.0, 0.0, 0.0]) - np.concatenate([[0.0], x[:-1]])
            d = nxt * rho * d + 2.0 * nxt / delta * res
            rho = nxt
    return [float(c) for c in x]


CHEB = cheb_weights()

ROUNDS = [(1, 1), (1, 0), (0, 1), (1, 1), (1, 0), (1, 1), (1, 0), (0, 2), (0, 1), (0, 1), (0, 1)]


def round_offsets():
    face, corner, out = 0, 0, []
    for fine, coarse in ROUNDS:
        out.append((face, corner))
        face += 80 * fine + 24 * coarse
        corner += 8 * (fine + coarse)
    return out, face, corner


OFFSETS, FACE_ROWS, CORNER_ROWS = round_offsets()


def kernel(nx, ny, src, cond, absn, smooth_ref, corr, *s):
    (raw, gbuf, split_index, fxy, f0, f4, mass, inv, load, u0, u1, u2, pa, first, pb, ca, cb, last, tmp,
     cfxy, cf0, cf2, cmass, cinv, rl, cfirst, qa, qb, ra0, ra1, ra2, w0, w1, wa, wb, wc, base,
     s1, s2, s3, s4, ar1, ar2, arx, ary, sface, rface, scorner, rcorner,
     in_sem, send_sem, recv_sem, ax_send, ax_recv, ay_send, ay_recv) = s
    x, y = lax.axis_index("gx"), lax.axis_index("gy")

    for a, ref in enumerate((src, cond, absn)):
        for t in range(5):
            pltpu.make_async_copy(ref.at[:, :, pl.ds(128 * t, 128)], raw.at[a, t], in_sem.at[a, t]).start()

    def x_peer(d):
        return (lax.rem(x + d + nx, nx), y)

    def y_peer(d):
        return (x, lax.rem(y + d + ny, ny))

    barrier = pltpu.get_barrier_semaphore()
    greeted = [(lax.rem(x + dx + nx, nx), lax.rem(y + dy + ny, ny)) for dx, dy in DIRS[4:]]
    greeted += [x_peer(d) for d in range(1, nx)] + [y_peer(d) for d in range(1, ny)]
    for peer in greeted:
        pl.semaphore_signal(barrier, inc=1, device_id=peer, device_id_type=MESH)

    lf = Level(5, fxy, f0, f4, mass, inv)
    lc = Level(3, cfxy, cf0, cf2, cmass, cinv)
    bufs, sems, ids = (sface, rface, scorner, rcorner), (send_sem, recv_sem), (x, y, nx, ny)
    rounds = []

    def exchange(index, *fields, forward=False):
        assert ROUNDS[index] == (sum(lv.q == 5 for lv, _ in fields), sum(lv.q == 3 for lv, _ in fields))
        e = Exchange(index, fields, OFFSETS[index], bufs, sems, ids, forward)
        rounds.append(e)
        e.start()
        return e

    lanes = Lanes(5)
    for t in range(5):
        split_index[t] = lanes.split_index[t]

    def read(a, ref, store):
        load_field(lanes, ref, raw.at[a], split_index, gbuf, in_sem.at[a], store)

    def store_flux(i, j, p):
        put(f0, lf.edge(i, j), p[0])
        put(f4, lf.edge(i, j), p[4])
        put(fxy, lf.at(i, j, 0), p[0] + down(p[4]))
        for k in range(1, 4):
            put(fxy, lf.at(i, j, k), p[k])

    def store_plain(ref):
        def store(i, j, p):
            put(ref, lf.at(i, j, 0), p[0] + down(p[4]))
            for k in range(1, 4):
                put(ref, lf.at(i, j, k), p[k])

        return store

    read(0, src, store_plain(load))
    restrict_y(lf, load, tmp)
    join_planes_y(lf, load)
    join_planes_x(lf, load)
    restrict_xz(lc, tmp, rl)
    read(1, cond, store_flux)
    pl.semaphore_wait(barrier, len(greeted))
    e_load = exchange(0, (lf, load), (lc, rl))
    read(2, absn, store_plain(mass))
    for i in range(3):
        for j in range(3):
            ratio = WC[i] * WC[j] / (WF[2 * i] * WF[2 * j])
            ends, mid = ratio * WC[0] / WF[0], ratio * WC[1] / WF[2]
            put(cf0, lc.edge(i, j), ends * row(f0, lf.edge(2 * i, 2 * j)))
            put(cf2, lc.edge(i, j), ends * row(f4, lf.edge(2 * i, 2 * j)))
            for a, b in ((cfxy, fxy), (cmass, mass)):
                put(a, lc.at(i, j, 0), ends * row(b, lf.at(2 * i, 2 * j, 0)))
                put(a, lc.at(i, j, 1), mid * row(b, lf.at(2 * i, 2 * j, 2)))
    local_diag(lf, inv)
    e_diag = exchange(1, (lf, inv))
    local_diag(lc, cinv)
    e_cdiag = exchange(2, (lc, cinv))

    def invert(lv):
        def body(i):
            for n in range(lv.q * lv.kz):
                p = lv.at(i, 0, 0) + n * 16
                put(lv.inv, p, 1.0 / row(lv.inv, p))

        unrolled(lv.q, body)

    e_load.finish()
    apply_local(lf, pa, load)
    apply_local(lc, qa, rl)
    e_pa = exchange(3, (lf, pa), (lc, qa))
    e_diag.finish()
    invert(lf)
    apply_local(lf, ca, u0, scaled=load, restrict=tmp)
    e_ca = exchange(4, (lf, ca))
    restrict_xz(lc, tmp, ra0)
    e_cdiag.finish()
    invert(lc)
    e_pa.finish()
    apply_local(lf, pb, first, scaled=pa, sums=s1)
    apply_local(lc, qb, cfirst, scaled=qa, sums=s3)
    e_pb = exchange(5, (lf, pb), (lc, qb), forward=True)
    e_ca.finish()
    apply_local(lf, cb, u1, scaled=ca, restrict=tmp)
    e_cb = exchange(6, (lf, cb))
    restrict_xz(lc, tmp, ra1)
    e_ra01 = exchange(7, (lc, ra0), (lc, ra1))
    e_pb.finish()
    sum_squares(lf, pb, s2)
    sum_squares(lc, qb, s4)

    def fold(sums):
        return jnp.sum(sums[...], axis=0, keepdims=True)

    def to_all(source, slots, count, peer, send, recv):
        copies = []
        for d in range(1, count):
            copy = pltpu.make_async_remote_copy(
                src_ref=source, dst_ref=slots.at[d], send_sem=send.at[d], recv_sem=recv.at[d], device_id=peer(d), device_id_type=MESH
            )
            copy.start()
            copies.append(copy)
        return copies

    def gathered(source, slots, count, copies):
        for copy in copies:
            copy.wait_recv()
        total = source[...]
        for d in range(1, count):
            total = total + slots[d]
        return total

    ar1[...] = jnp.concatenate([fold(s1), fold(s2), fold(s3), fold(s4), jnp.zeros((4, 128), F32)], axis=0)
    x_copies = to_all(ar1, arx, nx, x_peer, ax_send, ax_recv)

    e_cb.finish()
    apply_local(lf, last, u2, scaled=cb, restrict=tmp, keep=False)
    restrict_xz(lc, tmp, ra2)
    e_ra2 = exchange(8, (lc, ra2))
    ar2[...] = gathered(ar1, arx, nx, x_copies)
    y_copies = to_all(ar2, ary, ny, y_peer, ay_send, ay_recv)
    e_ra01.finish()
    e_ra2.finish()
    totals = jnp.sum(gathered(ar2, ary, ny, y_copies), axis=1, keepdims=True)

    def inverse_estimate(n):
        estimate = jnp.sqrt(totals[n + 1 : n + 2] / (totals[n : n + 1] + 1e-06))
        return jnp.broadcast_to(1.0 / estimate, (16, 128))

    g, gc = inverse_estimate(0), inverse_estimate(2)

    def horner(scale, a, b, c):
        return scale * (CHEB[0] * a + scale * (CHEB[1] * b + scale * (CHEB[2] * c)))

    for n in range(18):
        p = 16 * n
        put(wa, p, row(rl, p) - horner(g, row(ra0, p), row(ra1, p), row(ra2, p)))
    apply_local(lc, wb, w0, scaled=wa)
    e_w0 = exchange(9, (lc, wb))

    def smooth(i):
        for n in range(20):
            p = lf.at(i, 0, 0) + 16 * n
            put(smooth_ref, p, horner(g, row(u0, p), row(u1, p), row(u2, p)))

    loop(5, smooth)
    e_w0.finish()
    apply_local(lc, wc, w1, scaled=wb)
    e_w1 = exchange(10, (lc, wc))
    for n in range(18):
        p = 16 * n
        put(base, p, gc * (CHEB[0] * row(w0, p) + gc * (CHEB[1] * row(w1, p))))
    e_w1.finish()
    for n in range(18):
        p = 16 * n
        put(corr, p, row(base, p) + gc * (gc * (gc * (CHEB[2] * row(wc, p) * row(cinv, p)))))

    for e in rounds:
        e.wait_sent()
    for copy in x_copies + y_copies:
        copy.wait_send()


def lift(smooth_ref, corr, out_ref, corr_ref, gbuf, obuf, cbuf, merge_index, tmp, out_sem, cout_sem):
    lanes = Lanes(5)
    for t in range(5):
        merge_index[t] = lanes.merge_index[t]

    for i in range(3):
        lines = []
        for j in range(3):
            a, b = row(corr, ((i * 3 + j) * 2) * 16), row(corr, ((i * 3 + j) * 2 + 1) * 16)
            c = up(a)
            lines.append([a, JA * a + JB * b + JC * c, b, JC * a + JB * b + JA * c])
        for k in range(4):
            a, b, c = lines[0][k], lines[1][k], lines[2][k]
            for j, v in enumerate([a, JA * a + JB * b + JC * c, b, JC * a + JB * b + JA * c, c]):
                put(tmp, ((i * 5 + j) * 4 + k) * 16, v)

    def finish_plane(i):
        cx = [pick(i, [r[c] for r in JROWS]) for c in range(3)]
        for j in range(5):
            planes = []
            for k in range(4):
                lifted = [row(tmp, ((c * 5 + j) * 4 + k) * 16) for c in range(3)]
                lifted = cx[0] * lifted[0] + cx[1] * lifted[1] + cx[2] * lifted[2]
                planes.append(row(smooth_ref, ((i * 5 + j) * 4 + k) * 16) + lifted)
            planes.append(up(planes[0]))
            for h in range(2):
                for t, v in enumerate(lanes.mix([v[8 * h : 8 * h + 8] for v in planes])):
                    gbuf[t, pl.ds(pl.multiple_of((i * 5 + j) * 16 + 8 * h, 8), 8), :] = v

    def out_copy(t):
        return pltpu.make_async_copy(obuf.at[t], out_ref.at[:, :, pl.ds(pl.multiple_of(128 * t, 128), 128)], out_sem.at[t])

    def finish_tile(t):
        order = merge_index[t]
        for i in range(5):
            for j in range(5):
                for h in range(2):
                    stored = lanes.gather(gbuf[t, pl.ds((i * 5 + j) * 16 + 8 * h, 8), :], order)
                    obuf[t, 10 * h + i, pl.ds(j, 4, 5), :] = stored[:4]
                    obuf[t, 10 * h + 5 + i, pl.ds(j, 4, 5), :] = stored[4:]
        out_copy(t).start()

    loop(5, finish_plane)
    loop(5, finish_tile)

    thirds = Lanes(3)
    for i in range(3):
        for j in range(3):
            c = [row(corr, ((i * 3 + j) * 2) * 16), row(corr, ((i * 3 + j) * 2 + 1) * 16)]
            c.append(up(c[0]))
            for h in range(2):
                for t, v in enumerate(thirds.mix([v[8 * h : 8 * h + 8] for v in c])):
                    stored = thirds.gather(v, thirds.merge_index[t])
                    cbuf[t, 6 * h + i, pl.ds(j, 4, 3), :] = stored[:4]
                    cbuf[t, 6 * h + 3 + i, pl.ds(j, 4, 3), :] = stored[4:]
    copies = []
    for t in range(3):
        copy = pltpu.make_async_copy(cbuf.at[t], corr_ref.at[:, :, pl.ds(128 * t, 128)], cout_sem.at[t])
        copy.start()
        copies.append(copy)
    copies += [out_copy(t) for t in range(5)]
    for copy in copies:
        copy.wait()


def scratch(nx, ny):
    def v(*shape):
        return pltpu.VMEM(shape, F32)

    fine, coarse = v(FR, 128), v(CR, 128)
    dma = pltpu.SemaphoreType.DMA
    return (
        [v(3, 5, 20, 20, 128), v(5, 400, 128), pltpu.VMEM((5, 8, 128), jnp.int32)]
        + [fine, v(ER, 128), v(ER, 128)]
        + [fine] * 12
        + [v(960, 128)]
        + [coarse, v(CER, 128), v(CER, 128)]
        + [coarse] * 15
        + [v(16, 128)] * 4
        + [v(8, 128), v(8, 128), v(nx, 8, 128), v(ny, 8, 128)]
        + [v(4, FACE_ROWS, 128)] * 2
        + [v(4, CORNER_ROWS, 128)] * 2
        + [dma((3, 5)), dma((len(ROUNDS), 8)), dma((len(ROUNDS), 8))]
        + [dma((nx,)), dma((nx,)), dma((ny,)), dma((ny,))]
    )


def solution(mesh):
    nx, ny = mesh.shape["gx"], mesh.shape["gy"]

    def on_device(source, conductivity, absorption):
        vmem, hbm = pl.BlockSpec(memory_space=pltpu.VMEM), pl.BlockSpec(memory_space=pltpu.HBM)
        parts = pl.pallas_call(
            functools.partial(kernel, nx, ny),
            out_shape=(jax.ShapeDtypeStruct((FR, 128), F32), jax.ShapeDtypeStruct((CR, 128), F32)),
            in_specs=[hbm] * 3,
            out_specs=[vmem] * 2,
            scratch_shapes=scratch(nx, ny),
            compiler_params=pltpu.CompilerParams(collective_id=0, has_side_effects=True, vmem_limit_bytes=105 * 512 * 1024),
            name="window",
        )(source, conductivity, absorption)
        return pl.pallas_call(
            lift,
            out_shape=(jax.ShapeDtypeStruct((20, 20, 640), F32), jax.ShapeDtypeStruct((12, 12, 384), F32)),
            in_specs=[vmem] * 2,
            out_specs=[hbm] * 2,
            scratch_shapes=[
                pltpu.VMEM((5, 400, 128), F32),
                pltpu.VMEM((5, 20, 20, 128), F32),
                pltpu.VMEM((3, 12, 12, 128), F32),
                pltpu.VMEM((5, 8, 128), jnp.int32),
                pltpu.VMEM((960, 128), F32),
                pltpu.SemaphoreType.DMA((5,)),
                pltpu.SemaphoreType.DMA((3,)),
            ],
            compiler_params=pltpu.CompilerParams(vmem_limit_bytes=16 * 1024 * 1024),
            name="lift",
        )(*parts)

    placed = P("gx", "gy", None)
    return jax.shard_map(on_device, mesh=mesh, in_specs=(placed,) * 3, out_specs=(placed, placed), check_vma=False)
```

```python
import functools
import math

import jax
import jax.numpy as jnp
import numpy as np
from jax import lax
from jax.experimental import pallas as pl
from jax.experimental.pallas import tpu as pltpu
from jax.sharding import PartitionSpec as P

MESH = pl.DeviceIdType.MESH
SWEEPS = 3
F32 = jnp.float32


def deriv_table(points):
    count = len(points)
    bary = [1.0 / np.prod([points[j] - points[k] for k in range(count) if k != j]) for j in range(count)]
    table = np.zeros((count, count))
    for i in range(count):
        for j in range(count):
            if i != j:
                table[i, j] = bary[j] / (bary[i] * (points[i] - points[j]))
        table[i, i] = -np.sum(table[i])
    return table


ROOT = math.sqrt(3.0 / 7.0)
WF = [0.1, 49.0 / 90.0, 32.0 / 45.0, 49.0 / 90.0, 0.1]
WC = [1.0 / 3.0, 4.0 / 3.0, 1.0 / 3.0]
DF = deriv_table(np.array([-1.0, -ROOT, 0.0, ROOT, 1.0]))
JA, JB, JC = (ROOT * ROOT + ROOT) / 2, 1 - ROOT * ROOT, (ROOT * ROOT - ROOT) / 2
JROWS = [[1.0, 0.0, 0.0], [JA, JB, JC], [0.0, 1.0, 0.0], [JC, JB, JA], [0.0, 0.0, 1.0]]


B00, B01 = (DF[4][4] + DF[0][4]) / 2, (DF[4][3] + DF[0][3]) / 2
B10, B11 = (DF[3][4] + DF[1][4]) / 2, (DF[3][3] + DF[1][3]) / 2
G00, G01 = (DF[4][4] - DF[0][4]) / 2, (DF[4][3] - DF[0][3]) / 2
G10, G11 = (DF[3][4] - DF[1][4]) / 2, (DF[3][3] - DF[1][3]) / 2
A0, A1 = DF[2][4], DF[2][3]


def stiff5(v, flux):
    a0, a1 = v[4] - v[0], v[3] - v[1]
    m2 = v[2] + v[2]
    s0, s1 = v[0] + v[4] - m2, v[1] + v[3] - m2
    p0, p1 = B00 * a0 + B01 * a1, B10 * a0 + B11 * a1
    q0, q1 = G00 * s0 + G01 * s1, G10 * s0 + G11 * s1
    f0, f4 = flux[0] * (p0 - q0), flux[4] * (p0 + q0)
    f1, f3 = flux[1] * (p1 - q1), flux[3] * (p1 + q1)
    f2 = flux[2] * (A0 * a0 + A1 * a1)
    sp0, sq0, sp1, sq1 = f4 + f0, f4 - f0, f3 + f1, f3 - f1
    b0 = A0 * f2 + B00 * sp0 + B10 * sp1
    b1 = A1 * f2 + B01 * sp0 + B11 * sp1
    c0, c1 = G00 * sq0 + G10 * sq1, G01 * sq0 + G11 * sq1
    mid = c0 + c1
    return [c0 - b0, c1 - b1, -(mid + mid), c1 + b1, c0 + b0]


DD = (DF * DF).T


def diag5(flux):
    s0, s1, d0, d1 = flux[0] + flux[4], flux[1] + flux[3], flux[0] - flux[4], flux[1] - flux[3]
    out = [None] * 5
    for r in (0, 1):
        even = (DD[r][0] + DD[r][4]) / 2 * s0 + (DD[r][1] + DD[r][3]) / 2 * s1 + DD[r][2] * flux[2]
        odd = (DD[r][0] - DD[r][4]) / 2 * d0 + (DD[r][1] - DD[r][3]) / 2 * d1
        out[r], out[4 - r] = even + odd, even - odd
    out[2] = DD[2][0] * s0 + DD[2][1] * s1
    return out


def stiff3(v, flux):
    a = 0.5 * (v[2] - v[0])
    s = v[0] + v[2] - (v[1] + v[1])
    f0, f1, f2 = flux[0] * (a - s), flux[1] * a, flux[2] * (a + s)
    b = 0.5 * (f0 + f1 + f2)
    t = f2 - f0
    return [t - b, -(t + t), t + b]


DC = deriv_table(np.array([-1.0, 0.0, 1.0]))
DDC = (DC * DC).T


def diag3(flux):
    s = flux[0] + flux[2]
    return [
        DDC[0][0] * flux[0] + DDC[0][1] * flux[1] + DDC[0][2] * flux[2],
        DDC[1][0] * s,
        DDC[2][0] * flux[0] + DDC[2][1] * flux[1] + DDC[2][2] * flux[2],
    ]


def restrict5(y):
    return [y[0] + JA * y[1] + JC * y[3], JB * (y[1] + y[3]) + y[2], y[4] + JC * y[1] + JA * y[3]]


def up(x):
    return pltpu.roll(x, 127, 1)


def down(x):
    return pltpu.roll(x, 1, 1)


def loop(count, body):
    def step(i, carry):
        body(i)
        return carry

    lax.fori_loop(0, count, step, 0)


def unrolled(count, body):
    for i in range(count):
        body(i)


class Level:
    def __init__(self, q, fxy, f0, fq, mass, inv):
        self.q, self.kz = q, q - 1
        self.fxy, self.f0, self.fq, self.mass, self.inv = fxy, f0, fq, mass, inv
        self.stiff, self.diag = (stiff5, diag5) if q == 5 else (stiff3, diag3)
        self.face = q * self.kz * 4

    def at(self, i, j, k):
        return ((i * self.q + j) * self.kz + k) * 16

    def edge(self, i, j):
        return (i * self.q + j) * 16


def row(ref, start):
    if not isinstance(start, int):
        start = pl.multiple_of(start, 16)
    return ref[pl.ds(start, 16), :]


def put(ref, start, value):
    if not isinstance(start, int):
        start = pl.multiple_of(start, 16)
    ref[pl.ds(start, 16), :] = value


def element_rows():
    e = lax.broadcasted_iota(jnp.int32, (16, 128), 0)
    return e // 4, e % 4


def join_y(lo, hi):
    _, ey = element_rows()
    hi = hi + jnp.where(ey < 3, pltpu.roll(lo, 15, 0), 0.0)
    return jnp.where(ey > 0, pltpu.roll(hi, 1, 0), lo), hi


def join_x(lo, hi):
    ex, _ = element_rows()
    hi = hi + jnp.where(ex < 3, pltpu.roll(lo, 12, 0), 0.0)
    return jnp.where(ex > 0, pltpu.roll(hi, 4, 0), lo), hi


def join_planes_x(lv, out):
    q, kz = lv.q, lv.kz

    def body(j):
        for k in range(kz):
            lo, hi = join_x(row(out, lv.at(0, j, k)), row(out, lv.at(q - 1, j, k)))
            put(out, lv.at(0, j, k), lo)
            put(out, lv.at(q - 1, j, k), hi)

    unrolled(q, body)


def join_planes_y(lv, out):
    q, kz = lv.q, lv.kz

    def body(i):
        for k in range(kz):
            lo, hi = join_y(row(out, lv.at(i, 0, k)), row(out, lv.at(i, q - 1, k)))
            put(out, lv.at(i, 0, k), lo)
            put(out, lv.at(i, q - 1, k), hi)

    unrolled(q, body)


def apply_local(lv, out, u, scaled=None, sums=None, restrict=None, keep=True):
    q, kz = lv.q, lv.kz

    def along_z(i):
        total = None
        for j in range(q):
            base = lv.at(i, j, 0)
            if scaled is None:
                v = [row(u, base + 16 * k) for k in range(kz)]
            else:
                v = [row(scaled, base + 16 * k) * row(lv.inv, base + 16 * k) for k in range(kz)]
                for k in range(kz):
                    put(u, base + 16 * k, v[k])
                if sums is not None:
                    part = v[0] * v[0]
                    part = part + part
                    for k in range(1, kz):
                        part = part + v[k] * v[k]
                    total = part if total is None else total + part
            flux = [row(lv.f0, lv.edge(i, j))] + [row(lv.fxy, base + 16 * k) for k in range(1, kz)] + [row(lv.fq, lv.edge(i, j))]
            g = lv.stiff(v + [up(v[0])], flux)
            g = [g[0] + down(g[kz])] + g[1:kz]
            for k in range(kz):
                put(out, base + 16 * k, g[k] + row(lv.mass, base + 16 * k) * v[k])
        if sums is not None:
            sums[...] += total

    def along_x(j):
        for k in range(kz):
            places = [lv.at(i, j, k) for i in range(q)]
            g = lv.stiff([row(u, p) for p in places], [row(lv.fxy, p) for p in places])
            for i in range(q):
                put(out, places[i], row(out, places[i]) + g[i])

    def along_y(i):
        for k in range(kz):
            places = [lv.at(i, j, k) for j in range(q)]
            g = lv.stiff([row(u, p) for p in places], [row(lv.fxy, p) for p in places])
            g = [row(out, places[j]) + g[j] for j in range(q)]
            if restrict is not None:
                c = restrict5(g)
                for jc in range(3):
                    put(restrict, ((i * 3 + jc) * 4 + k) * 16, c[jc])
            if keep:
                g[0], g[q - 1] = join_y(g[0], g[q - 1])
                for j in range(q):
                    put(out, places[j], g[j])

    if sums is not None:
        sums[...] = jnp.zeros_like(sums)
    unrolled(q, along_z)
    unrolled(q, along_x)
    unrolled(q, along_y)
    if keep:
        join_planes_x(lv, out)


def sum_squares(lv, scaled, sums):
    total = [None] * 4
    for i in range(lv.q - 1):
        for j in range(lv.q - 1):
            for k in range(lv.kz):
                p = lv.at(i, j, k)
                v = row(scaled, p) * row(lv.inv, p)
                v = v * v
                zeros = (i == 0) + (j == 0) + (k == 0)
                total[zeros] = v if total[zeros] is None else total[zeros] + v
    sums[...] = total[0] + 2.0 * total[1] + 4.0 * total[2] + 8.0 * total[3]


def restrict_xz(lc, tmp, out):
    for jc in range(3):
        cols = [restrict5([row(tmp, ((i * 3 + jc) * 4 + k) * 16) for i in range(5)]) for k in range(4)]
        for ic in range(3):
            y = [cols[k][ic] for k in range(4)]
            first = y[0] + JA * y[1] + JC * y[3] + down(JC * y[1] + JA * y[3])
            put(out, lc.at(ic, jc, 0), first)
            put(out, lc.at(ic, jc, 1), JB * (y[1] + y[3]) + y[2])
    join_planes_y(lc, out)
    join_planes_x(lc, out)


def restrict_y(lv, src, tmp):
    def body(i):
        for k in range(4):
            c = restrict5([row(src, lv.at(i, j, k)) for j in range(5)])
            for jc in range(3):
                put(tmp, ((i * 3 + jc) * 4 + k) * 16, c[jc])

    unrolled(5, body)


def local_diag(lv, out):
    q, kz = lv.q, lv.kz

    def along_z(i):
        for j in range(q):
            base = lv.at(i, j, 0)
            flux = [row(lv.f0, lv.edge(i, j))] + [row(lv.fxy, base + 16 * k) for k in range(1, kz)] + [row(lv.fq, lv.edge(i, j))]
            g = lv.diag(flux)
            g = [g[0] + down(g[kz])] + g[1:kz]
            for k in range(kz):
                put(out, base + 16 * k, g[k] + row(lv.mass, base + 16 * k))

    def along_x(j):
        for k in range(kz):
            places = [lv.at(i, j, k) for i in range(q)]
            g = lv.diag([row(lv.fxy, p) for p in places])
            for i in range(q):
                put(out, places[i], row(out, places[i]) + g[i])

    def along_y(i):
        for k in range(kz):
            places = [lv.at(i, j, k) for j in range(q)]
            g = lv.diag([row(lv.fxy, p) for p in places])
            g = [row(out, places[j]) + g[j] for j in range(q)]
            g[0], g[q - 1] = join_y(g[0], g[q - 1])
            for j in range(q):
                put(out, places[j], g[j])

    unrolled(q, along_z)
    unrolled(q, along_x)
    unrolled(q, along_y)
    join_planes_x(lv, out)


DIRS = [(0, 1), (0, -1), (1, 0), (-1, 0), (1, 1), (1, -1), (-1, 1), (-1, -1)]


def directions(forward):
    return [d for d, (dx, dy) in enumerate(DIRS) if not forward or (dx >= 0 and dy >= 0)]


def wait_all(ref, sem):
    pltpu.make_async_copy(ref, ref, sem).wait()


class Exchange:
    def __init__(self, round_index, fields, region, bufs, sems, ids, forward):
        self.r, self.fields, self.ids = round_index, fields, ids
        self.bufs, self.sems = bufs, sems
        face, corner = sum(lv.face for lv, _ in fields), 8 * len(fields)
        self.dirs = directions(forward)
        self.part, at = {}, region[0]
        for d in self.dirs:
            self.part[d] = (at, face if d < 4 else corner)
            at += self.part[d][1]
        assert at == region[0] + region[1]
        self.region = pl.ds(*region)

    def pack(self):
        sbuf = self.bufs[0]
        at = 0
        for f, (lv, ref) in enumerate(self.fields):
            q, kz = lv.q, lv.kz
            for d, (dx, dy) in enumerate(DIRS[:4]):
                if d not in self.dirs:
                    continue
                if dy:
                    j, first = (q - 1, 3) if dy > 0 else (0, 0)
                    for i in range(q):
                        for h in range(0, 4 * kz, 8):
                            sbuf[pl.ds(self.part[d][0] + at + i * 4 * kz + h, 8), :] = ref[pl.ds(lv.at(i, j, 0) + first + 4 * h, 8, 4), :]
                else:
                    i = q - 1 if dx > 0 else 0
                    low = lax.broadcasted_iota(jnp.int32, (8, 128), 0) < 4
                    for m in range(0, q * kz, 2):
                        p = lv.at(i, 0, 0) + m * 16
                        if dx > 0:
                            one, two = ref[pl.ds(p + 8, 8), :], ref[pl.ds(p + 24, 8), :]
                            both = jnp.where(low, pltpu.roll(one, 4, 0), two)
                        else:
                            one, two = ref[pl.ds(p, 8), :], ref[pl.ds(p + 16, 8), :]
                            both = jnp.where(low, one, pltpu.roll(two, 4, 0))
                        sbuf[pl.ds(self.part[d][0] + at + m * 4, 8), :] = both
            for c, (dx, dy) in enumerate(DIRS[4:]):
                if c + 4 not in self.dirs:
                    continue
                p = lv.at(q - 1 if dx > 0 else 0, q - 1 if dy > 0 else 0, 0) + (12 if dx > 0 else 0) + (3 if dy > 0 else 0)
                for k in range(kz):
                    sbuf[pl.ds(self.part[c + 4][0] + f * 8 + k, 1), :] = ref[pl.ds(p + 16 * k, 1), :]
            at += lv.face

    def send(self):
        sbuf, rbuf = self.bufs
        send_sem, recv_sem = self.sems
        x, y, nx, ny = self.ids
        for d in self.dirs:
            dx, dy = DIRS[d]
            part = pl.ds(*self.part[d])
            pltpu.make_async_remote_copy(
                src_ref=sbuf.at[part],
                dst_ref=rbuf.at[part],
                send_sem=send_sem.at[self.r],
                recv_sem=recv_sem.at[self.r],
                device_id=(lax.rem(x + dx + nx, nx), lax.rem(y + dy + ny, ny)),
                device_id_type=MESH,
            ).start()

    def start(self):
        self.pack()
        self.send()

    def finish(self):
        rbuf = self.bufs[1]
        wait_all(rbuf.at[self.region], self.sems[1].at[self.r])
        at = 0
        for f, (lv, ref) in enumerate(self.fields):
            q, kz = lv.q, lv.kz
            for d, (dx, dy) in enumerate(DIRS[:4]):
                if d not in self.dirs:
                    continue
                if dy:
                    j, first = (0, 0) if dy > 0 else (q - 1, 3)
                    for i in range(q):
                        for h in range(0, 4 * kz, 8):
                            place = pl.ds(lv.at(i, j, 0) + first + 4 * h, 8, 4)
                            ref[place, :] = ref[place, :] + rbuf[pl.ds(self.part[d][0] + at + i * 4 * kz + h, 8), :]
                else:
                    i = 0 if dx > 0 else q - 1
                    low = lax.broadcasted_iota(jnp.int32, (8, 128), 0) < 4
                    for m in range(0, q * kz, 2):
                        p = lv.at(i, 0, 0) + m * 16
                        both = rbuf[pl.ds(self.part[d][0] + at + m * 4, 8), :]
                        turned = pltpu.roll(both, 4, 0)
                        if dx > 0:
                            a, b = pl.ds(p, 8), pl.ds(p + 16, 8)
                            ref[a, :] = ref[a, :] + jnp.where(low, both, 0.0)
                            ref[b, :] = ref[b, :] + jnp.where(low, turned, 0.0)
                        else:
                            a, b = pl.ds(p + 8, 8), pl.ds(p + 24, 8)
                            ref[a, :] = ref[a, :] + jnp.where(low, 0.0, turned)
                            ref[b, :] = ref[b, :] + jnp.where(low, 0.0, both)
            for c, (dx, dy) in enumerate(DIRS[4:]):
                if c + 4 not in self.dirs:
                    continue
                p = lv.at(0 if dx > 0 else q - 1, 0 if dy > 0 else q - 1, 0) + (0 if dx > 0 else 12) + (0 if dy > 0 else 3)
                for k in range(kz):
                    place = pl.ds(p + 16 * k, 1)
                    ref[place, :] = ref[place, :] + rbuf[pl.ds(self.part[c + 4][0] + f * 8 + k, 1), :]
            at += lv.face

    def wait_sent(self):
        wait_all(self.bufs[0].at[self.region], self.sems[0].at[self.r])


class Lanes:
    def __init__(self, q):
        self.q = q
        step = {k: (k - 128) % q for k in range(q)}
        shift = {0: 0}
        k = 0
        for _ in range(q - 1):
            shift[step[k]] = shift[k] + self.begin(k, 1) - self.begin(step[k], 0)
            k = step[k]
        self.shift = [shift[k] % 128 for k in range(q)]
        lane = lax.broadcasted_iota(jnp.int32, (8, 128), 1)
        self.lane = lane
        self.split_index, self.merge_index = [], []
        for t in range(q):
            place = 128 * t + lane
            k = lax.rem(place, q)
            ez = lax.div(place, q)
            moved = ez
            for node in range(q):
                moved = jnp.where(k == node, ez + self.shift[node], moved)
            self.merge_index.append(jnp.bitwise_and(moved, 127))
            index = jnp.zeros((8, 128), jnp.int32)
            for node in range(q):
                ez = jnp.bitwise_and(lane - self.shift[node] + 128, 127)
                index = jnp.where(self.inside(node, t), q * ez + node - 128 * t, index)
            self.split_index.append(index)

    def begin(self, k, t):
        return -((k - 128 * t) // self.q)

    def inside(self, k, t):
        lo, hi = (self.begin(k, t) + self.shift[k]) % 128, (self.begin(k, t + 1) + self.shift[k]) % 128
        if lo < hi:
            return (self.lane >= lo) & (self.lane < hi) if lo else self.lane < hi
        return (self.lane >= lo) | (self.lane < hi) if hi else self.lane >= lo

    @staticmethod
    def gather(x, index):
        numbers = lax.GatherDimensionNumbers(
            offset_dims=(), collapsed_slice_dims=(1,), start_index_map=(1,), operand_batching_dims=(0,), start_indices_batching_dims=(0,)
        )
        return lax.gather(x, index[..., None], numbers, slice_sizes=(1, 1), mode=lax.GatherScatterMode.PROMISE_IN_BOUNDS)

    def unmix(self, moved):
        out = []
        for k in range(self.q):
            x = moved[0]
            for t in range(1, self.q):
                x = jnp.where(self.inside(k, t), moved[t], x)
            out.append(pltpu.roll(x, (128 - self.shift[k]) % 128, 1) if self.shift[k] else x)
        return out

    def mix(self, nodes):
        moved = [pltpu.roll(nodes[k], self.shift[k], 1) if self.shift[k] else nodes[k] for k in range(self.q)]
        out = []
        for t in range(self.q):
            x = moved[0]
            for k in range(1, self.q):
                x = jnp.where(self.inside(k, t), moved[k], x)
            out.append(x)
        return out


def pick(i, values):
    out = jnp.asarray(values[-1], F32)
    for n in range(len(values) - 2, -1, -1):
        out = jnp.where(i == n, jnp.asarray(values[n], F32), out)
    return out


def load_field(lanes, ref, raw, index, buf, sem, store):
    def tile(t):
        pltpu.make_async_copy(ref.at[:, :, pl.ds(pl.multiple_of(128 * t, 128), 128)], raw.at[t], sem.at[t]).wait()
        order = index[t]
        for i in range(5):
            for j in range(5):
                for h in range(2):
                    low = raw[t, 10 * h + i, pl.ds(j, 4, 5), :]
                    high = raw[t, 10 * h + 5 + i, pl.ds(j, 4, 5), :]
                    both = jnp.concatenate([low, high], axis=0)
                    buf[t, pl.ds((i * 5 + j) * 16 + 8 * h, 8), :] = lanes.gather(both, order)

    def plane(i):
        wx = pick(i, WF)
        for j in range(5):
            halves = []
            for h in range(2):
                p = pl.ds(pl.multiple_of((i * 5 + j) * 16 + 8 * h, 8), 8)
                halves.append(lanes.unmix([buf[t, p, :] for t in range(5)]))
            store(i, j, [jnp.concatenate([halves[0][k], halves[1][k]], axis=0) * (wx * (WF[j] * WF[k])) for k in range(5)])

    loop(5, tile)
    loop(5, plane)


FR, CR, ER, CER = 1600, 288, 400, 144


def cheb_weights():
    sigma, rho = 5.0 / 3.0, 0.6
    theta, delta = 0.75, 0.45
    d = np.array([1.0 / theta, 0.0, 0.0])
    x = np.zeros(3)
    for sweep in range(SWEEPS):
        x = x + d
        if sweep + 1 < SWEEPS:
            nxt = 1.0 / (2.0 * sigma - rho)
            res = np.array([1.0, 0.0, 0.0]) - np.concatenate([[0.0], x[:-1]])
            d = nxt * rho * d + 2.0 * nxt / delta * res
            rho = nxt
    return [float(c) for c in x]


CHEB = cheb_weights()

ROUNDS = [
    (1, 0, False), (1, 0, False), (0, 2, False), (1, 0, False), (1, 0, False), (0, 1, False), (1, 0, True), (0, 2, False),
    (0, 1, True), (1, 0, False), (0, 1, False), (0, 1, False), (0, 2, False), (0, 1, False), (0, 1, False),
]


def round_regions():
    at, out = 0, []
    for fine, coarse, forward in ROUNDS:
        sizes = [80 * fine + 24 * coarse if d < 4 else 8 * (fine + coarse) for d in directions(forward)]
        out.append((at, sum(sizes)))
        at += sum(sizes)
    return out, at


REGIONS, BUF_ROWS = round_regions()


def kernel(nx, ny, src, cond, absn, smooth_ref, corr, merge_index, *s):
    (raw, gbuf, split_index, fxy, f0, f4, mass, inv, load, u0, u1, u2, pa, first, pb, ca, cb, last, tmp,
     cfxy, cf0, cf2, cmass, cinv, rl, cfirst, qa, qb, ra0, ra1, ra2, vl, v0, v1, v2, al, a0, a1, a2, w0, w1, wa, wc, base,
     s1, s2, s3, s4, ar1, ar2, arx, ary, sbuf, rbuf, in_sem, send_sem, recv_sem, ar_send, ar_recv) = s
    x, y = lax.axis_index("gx"), lax.axis_index("gy")

    for a, ref in enumerate((src, cond, absn)):
        for t in range(5):
            pltpu.make_async_copy(ref.at[:, :, pl.ds(128 * t, 128)], raw.at[a, t], in_sem.at[a, t]).start()

    def x_peer(d):
        return (lax.rem(x + d + nx, nx), y)

    def y_peer(d):
        return (x, lax.rem(y + d + ny, ny))

    barrier = pltpu.get_barrier_semaphore()
    greeted = [(lax.rem(x + dx + nx, nx), lax.rem(y + dy + ny, ny)) for dx, dy in DIRS[4:]]
    greeted += [x_peer(d) for d in range(1, nx)] + [y_peer(d) for d in range(1, ny)]
    for peer in greeted:
        pl.semaphore_signal(barrier, inc=1, device_id=peer, device_id_type=MESH)

    lf = Level(5, fxy, f0, f4, mass, inv)
    lc = Level(3, cfxy, cf0, cf2, cmass, cinv)
    bufs, sems, ids = (sbuf, rbuf), (send_sem, recv_sem), (x, y, nx, ny)
    rounds = []

    def exchange(index, *fields, forward=False):
        e = Exchange(index, fields, REGIONS[index], bufs, sems, ids, forward)
        e.start()
        if len(rounds) >= 4:
            rounds[-4].wait_sent()
        rounds.append(e)
        return e

    lanes = Lanes(5)
    for t in range(5):
        split_index[t] = lanes.split_index[t]
        merge_index[t] = lanes.merge_index[t]

    def read(a, ref, store):
        load_field(lanes, ref, raw.at[a], split_index, gbuf, in_sem.at[a], store)

    def store_flux(i, j, p):
        put(f0, lf.edge(i, j), p[0])
        put(f4, lf.edge(i, j), p[4])
        put(fxy, lf.at(i, j, 0), p[0] + down(p[4]))
        for k in range(1, 4):
            put(fxy, lf.at(i, j, k), p[k])

    def store_plain(ref):
        def store(i, j, p):
            put(ref, lf.at(i, j, 0), p[0] + down(p[4]))
            for k in range(1, 4):
                put(ref, lf.at(i, j, k), p[k])

        return store

    read(0, src, store_plain(load))
    restrict_y(lf, load, tmp)
    join_planes_y(lf, load)
    join_planes_x(lf, load)
    restrict_xz(lc, tmp, rl)
    read(1, cond, store_flux)
    pl.semaphore_wait(barrier, len(greeted))
    e_load = exchange(0, (lf, load))
    read(2, absn, store_plain(mass))
    for i in range(3):
        for j in range(3):
            ratio = WC[i] * WC[j] / (WF[2 * i] * WF[2 * j])
            ends, mid = ratio * WC[0] / WF[0], ratio * WC[1] / WF[2]
            put(cf0, lc.edge(i, j), ends * row(f0, lf.edge(2 * i, 2 * j)))
            put(cf2, lc.edge(i, j), ends * row(f4, lf.edge(2 * i, 2 * j)))
            for a, b in ((cfxy, fxy), (cmass, mass)):
                put(a, lc.at(i, j, 0), ends * row(b, lf.at(2 * i, 2 * j, 0)))
                put(a, lc.at(i, j, 1), mid * row(b, lf.at(2 * i, 2 * j, 2)))
    local_diag(lf, inv)
    e_diag = exchange(1, (lf, inv))
    local_diag(lc, cinv)
    e_coarse = exchange(2, (lc, rl), (lc, cinv))

    def invert(lv):
        def body(i):
            for n in range(lv.q * lv.kz):
                p = lv.at(i, 0, 0) + n * 16
                put(lv.inv, p, 1.0 / row(lv.inv, p))

        unrolled(lv.q, body)

    e_load.finish()
    apply_local(lf, pa, load)
    e_pa = exchange(3, (lf, pa))
    e_diag.finish()
    invert(lf)
    apply_local(lf, ca, u0, scaled=load, restrict=tmp)
    e_ca = exchange(4, (lf, ca))
    restrict_xz(lc, tmp, ra0)
    e_coarse.finish()
    invert(lc)
    apply_local(lc, qa, rl)
    e_qa = exchange(5, (lc, qa))
    apply_local(lc, al, vl, scaled=rl)
    e_pa.finish()
    apply_local(lf, pb, first, scaled=pa, sums=s1)
    e_pb = exchange(6, (lf, pb), forward=True)
    e_al = exchange(7, (lc, ra0), (lc, al))
    e_qa.finish()
    apply_local(lc, qb, cfirst, scaled=qa, sums=s3)
    e_qb = exchange(8, (lc, qb), forward=True)
    e_ca.finish()
    apply_local(lf, cb, u1, scaled=ca, restrict=tmp)
    e_cb = exchange(9, (lf, cb))
    restrict_xz(lc, tmp, ra1)
    e_pb.finish()
    sum_squares(lf, pb, s2)
    e_qb.finish()
    sum_squares(lc, qb, s4)

    def fold(sums):
        return jnp.sum(sums[...], axis=0, keepdims=True)

    def to_all(phase, source, slots, count, peer):
        for d in range(1, count):
            pltpu.make_async_remote_copy(
                src_ref=source,
                dst_ref=slots.at[d],
                send_sem=ar_send.at[phase],
                recv_sem=ar_recv.at[phase],
                device_id=peer(d),
                device_id_type=MESH,
            ).start()

    def gathered(phase, source, slots, count):
        wait_all(slots.at[pl.ds(1, count - 1)], ar_recv.at[phase])
        total = source[...]
        for d in range(1, count):
            total = total + slots[d]
        wait_all(slots.at[pl.ds(1, count - 1)], ar_send.at[phase])
        return total

    ar1[...] = jnp.concatenate([fold(s1), fold(s2), fold(s3), fold(s4), jnp.zeros((4, 128), F32)], axis=0)
    to_all(0, ar1, arx, nx, x_peer)
    e_ra1 = exchange(10, (lc, ra1))
    e_al.finish()
    apply_local(lc, a0, v0, scaled=ra0)

    e_cb.finish()
    apply_local(lf, last, u2, scaled=cb, restrict=tmp, keep=False)
    restrict_xz(lc, tmp, ra2)
    e_ra2 = exchange(11, (lc, ra2))
    e_ra1.finish()
    apply_local(lc, a1, v1, scaled=ra1)
    ar2[...] = gathered(0, ar1, arx, nx)
    to_all(1, ar2, ary, ny, y_peer)
    e_a01 = exchange(12, (lc, a0), (lc, a1))
    e_ra2.finish()
    apply_local(lc, a2, v2, scaled=ra2)
    e_a2 = exchange(13, (lc, a2))
    e_a01.finish()
    totals = jnp.sum(gathered(1, ar2, ary, ny), axis=1, keepdims=True)

    def inverse_estimate(n):
        estimate = jnp.sqrt(totals[n + 1 : n + 2] / (totals[n : n + 1] + 1e-06))
        return jnp.broadcast_to(1.0 / estimate, (16, 128))

    g, gc = inverse_estimate(0), inverse_estimate(2)

    def horner(scale, a, b, c):
        return scale * (CHEB[0] * a + scale * (CHEB[1] * b + scale * (CHEB[2] * c)))

    for n in range(18):
        p = 16 * n
        put(w0, p, row(vl, p) - horner(g, row(v0, p), row(v1, p), row(v2, p)))
        put(wa, p, row(al, p) - g * (CHEB[0] * row(a0, p) + g * (CHEB[1] * row(a1, p))))

    def smooth(i):
        for n in range(20):
            p = lf.at(i, 0, 0) + 16 * n
            put(smooth_ref, p, horner(g, row(u0, p), row(u1, p), row(u2, p)))

    loop(5, smooth)
    e_a2.finish()
    for n in range(18):
        p = 16 * n
        put(wa, p, row(wa, p) - g * (g * (g * (CHEB[2] * row(a2, p)))))
    apply_local(lc, wc, w1, scaled=wa)
    e_w1 = exchange(14, (lc, wc))
    for n in range(18):
        p = 16 * n
        put(base, p, gc * (CHEB[0] * row(w0, p) + gc * (CHEB[1] * row(w1, p))))
    e_w1.finish()
    for n in range(18):
        p = 16 * n
        put(corr, p, row(base, p) + gc * (gc * (gc * (CHEB[2] * row(wc, p) * row(cinv, p)))))

    for e in rounds[-4:]:
        e.wait_sent()


def lift(smooth_ref, corr, merge_index, out_ref, corr_ref, gbuf, obuf, cbuf, tmp, out_sem, cout_sem):
    lanes = Lanes(5)

    for i in range(3):
        lines = []
        for j in range(3):
            a, b = row(corr, ((i * 3 + j) * 2) * 16), row(corr, ((i * 3 + j) * 2 + 1) * 16)
            c = up(a)
            lines.append([a, JA * a + JB * b + JC * c, b, JC * a + JB * b + JA * c])
        for k in range(4):
            a, b, c = lines[0][k], lines[1][k], lines[2][k]
            for j, v in enumerate([a, JA * a + JB * b + JC * c, b, JC * a + JB * b + JA * c, c]):
                put(tmp, ((i * 5 + j) * 4 + k) * 16, v)

    def finish_plane(i):
        cx = [pick(i, [r[c] for r in JROWS]) for c in range(3)]
        for j in range(5):
            planes = []
            for k in range(4):
                lifted = [row(tmp, ((c * 5 + j) * 4 + k) * 16) for c in range(3)]
                lifted = cx[0] * lifted[0] + cx[1] * lifted[1] + cx[2] * lifted[2]
                planes.append(row(smooth_ref, ((i * 5 + j) * 4 + k) * 16) + lifted)
            planes.append(up(planes[0]))
            for h in range(2):
                for t, v in enumerate(lanes.mix([v[8 * h : 8 * h + 8] for v in planes])):
                    gbuf[t, pl.ds(pl.multiple_of((i * 5 + j) * 16 + 8 * h, 8), 8), :] = v

    def out_copy(t):
        return pltpu.make_async_copy(obuf.at[t], out_ref.at[:, :, pl.ds(pl.multiple_of(128 * t, 128), 128)], out_sem.at[t])

    def finish_tile(t):
        order = merge_index[t]
        for i in range(5):
            for j in range(5):
                for h in range(2):
                    stored = lanes.gather(gbuf[t, pl.ds((i * 5 + j) * 16 + 8 * h, 8), :], order)
                    obuf[t, 10 * h + i, pl.ds(j, 4, 5), :] = stored[:4]
                    obuf[t, 10 * h + 5 + i, pl.ds(j, 4, 5), :] = stored[4:]
        out_copy(t).start()

    loop(5, finish_plane)
    loop(5, finish_tile)

    thirds = Lanes(3)
    for i in range(3):
        for j in range(3):
            c = [row(corr, ((i * 3 + j) * 2) * 16), row(corr, ((i * 3 + j) * 2 + 1) * 16)]
            c.append(up(c[0]))
            for h in range(2):
                for t, v in enumerate(thirds.mix([v[8 * h : 8 * h + 8] for v in c])):
                    stored = thirds.gather(v, thirds.merge_index[t])
                    cbuf[t, 6 * h + i, pl.ds(j, 4, 3), :] = stored[:4]
                    cbuf[t, 6 * h + 3 + i, pl.ds(j, 4, 3), :] = stored[4:]
    copies = []
    for t in range(3):
        copy = pltpu.make_async_copy(cbuf.at[t], corr_ref.at[:, :, pl.ds(128 * t, 128)], cout_sem.at[t])
        copy.start()
        copies.append(copy)
    copies += [out_copy(t) for t in range(5)]
    for copy in copies:
        copy.wait()


def scratch(nx, ny):
    def v(*shape):
        return pltpu.VMEM(shape, F32)

    fine, coarse = v(FR, 128), v(CR, 128)
    dma = pltpu.SemaphoreType.DMA
    return (
        [v(3, 5, 20, 20, 128), v(5, 400, 128), pltpu.VMEM((5, 8, 128), jnp.int32)]
        + [fine, v(ER, 128), v(ER, 128)]
        + [fine] * 12
        + [v(960, 128)]
        + [coarse, v(CER, 128), v(CER, 128)]
        + [coarse] * 22
        + [v(16, 128)] * 4
        + [v(8, 128), v(8, 128), v(nx, 8, 128), v(ny, 8, 128)]
        + [v(BUF_ROWS, 128)] * 2
        + [dma((3, 5)), dma((len(ROUNDS),)), dma((len(ROUNDS),)), dma((2,)), dma((2,))]
    )


def solution(mesh):
    nx, ny = mesh.shape["gx"], mesh.shape["gy"]

    def on_device(source, conductivity, absorption):
        vmem, hbm = pl.BlockSpec(memory_space=pltpu.VMEM), pl.BlockSpec(memory_space=pltpu.HBM)
        parts = pl.pallas_call(
            functools.partial(kernel, nx, ny),
            out_shape=(jax.ShapeDtypeStruct((FR, 128), F32), jax.ShapeDtypeStruct((CR, 128), F32), jax.ShapeDtypeStruct((5, 8, 128), jnp.int32)),
            in_specs=[hbm] * 3,
            out_specs=[vmem] * 3,
            scratch_shapes=scratch(nx, ny),
            compiler_params=pltpu.CompilerParams(collective_id=0, has_side_effects=True, vmem_limit_bytes=105 * 512 * 1024),
            name="window",
        )(source, conductivity, absorption)
        return pl.pallas_call(
            lift,
            out_shape=(jax.ShapeDtypeStruct((20, 20, 640), F32), jax.ShapeDtypeStruct((12, 12, 384), F32)),
            in_specs=[vmem] * 3,
            out_specs=[hbm] * 2,
            scratch_shapes=[
                pltpu.VMEM((5, 400, 128), F32),
                pltpu.VMEM((5, 20, 20, 128), F32),
                pltpu.VMEM((3, 12, 12, 128), F32),
                pltpu.VMEM((960, 128), F32),
                pltpu.SemaphoreType.DMA((5,)),
                pltpu.SemaphoreType.DMA((3,)),
            ],
            compiler_params=pltpu.CompilerParams(vmem_limit_bytes=16 * 1024 * 1024),
            name="lift",
        )(*parts)

    placed = P("gx", "gy", None)
    return jax.shard_map(on_device, mesh=mesh, in_specs=(placed,) * 3, out_specs=(placed, placed), check_vma=False)
```

```python
import functools
import math

import jax
import jax.numpy as jnp
import numpy as np
from jax import lax
from jax.experimental import pallas as pl
from jax.experimental.pallas import tpu as pltpu
from jax.sharding import PartitionSpec as P

MESH = pl.DeviceIdType.MESH
SWEEPS = 3
F32 = jnp.float32


def deriv_table(points):
    count = len(points)
    bary = [1.0 / np.prod([points[j] - points[k] for k in range(count) if k != j]) for j in range(count)]
    table = np.zeros((count, count))
    for i in range(count):
        for j in range(count):
            if i != j:
                table[i, j] = bary[j] / (bary[i] * (points[i] - points[j]))
        table[i, i] = -np.sum(table[i])
    return table


ROOT = math.sqrt(3.0 / 7.0)
WF = [0.1, 49.0 / 90.0, 32.0 / 45.0, 49.0 / 90.0, 0.1]
WC = [1.0 / 3.0, 4.0 / 3.0, 1.0 / 3.0]
DF = deriv_table(np.array([-1.0, -ROOT, 0.0, ROOT, 1.0]))
JA, JB, JC = (ROOT * ROOT + ROOT) / 2, 1 - ROOT * ROOT, (ROOT * ROOT - ROOT) / 2
JROWS = [[1.0, 0.0, 0.0], [JA, JB, JC], [0.0, 1.0, 0.0], [JC, JB, JA], [0.0, 0.0, 1.0]]


B00, B01 = (DF[4][4] + DF[0][4]) / 2, (DF[4][3] + DF[0][3]) / 2
B10, B11 = (DF[3][4] + DF[1][4]) / 2, (DF[3][3] + DF[1][3]) / 2
G00, G01 = (DF[4][4] - DF[0][4]) / 2, (DF[4][3] - DF[0][3]) / 2
G10, G11 = (DF[3][4] - DF[1][4]) / 2, (DF[3][3] - DF[1][3]) / 2
A0, A1 = DF[2][4], DF[2][3]


def stiff5(v, flux):
    a0, a1 = v[4] - v[0], v[3] - v[1]
    m2 = v[2] + v[2]
    s0, s1 = v[0] + v[4] - m2, v[1] + v[3] - m2
    p0, p1 = B00 * a0 + B01 * a1, B10 * a0 + B11 * a1
    q0, q1 = G00 * s0 + G01 * s1, G10 * s0 + G11 * s1
    f0, f4 = flux[0] * (p0 - q0), flux[4] * (p0 + q0)
    f1, f3 = flux[1] * (p1 - q1), flux[3] * (p1 + q1)
    f2 = flux[2] * (A0 * a0 + A1 * a1)
    sp0, sq0, sp1, sq1 = f4 + f0, f4 - f0, f3 + f1, f3 - f1
    b0 = A0 * f2 + B00 * sp0 + B10 * sp1
    b1 = A1 * f2 + B01 * sp0 + B11 * sp1
    c0, c1 = G00 * sq0 + G10 * sq1, G01 * sq0 + G11 * sq1
    mid = c0 + c1
    return [c0 - b0, c1 - b1, -(mid + mid), c1 + b1, c0 + b0]


DD = (DF * DF).T


def diag5(flux):
    s0, s1, d0, d1 = flux[0] + flux[4], flux[1] + flux[3], flux[0] - flux[4], flux[1] - flux[3]
    out = [None] * 5
    for r in (0, 1):
        even = (DD[r][0] + DD[r][4]) / 2 * s0 + (DD[r][1] + DD[r][3]) / 2 * s1 + DD[r][2] * flux[2]
        odd = (DD[r][0] - DD[r][4]) / 2 * d0 + (DD[r][1] - DD[r][3]) / 2 * d1
        out[r], out[4 - r] = even + odd, even - odd
    out[2] = DD[2][0] * s0 + DD[2][1] * s1
    return out


def stiff3(v, flux):
    a = 0.5 * (v[2] - v[0])
    s = v[0] + v[2] - (v[1] + v[1])
    f0, f1, f2 = flux[0] * (a - s), flux[1] * a, flux[2] * (a + s)
    b = 0.5 * (f0 + f1 + f2)
    t = f2 - f0
    return [t - b, -(t + t), t + b]


DC = deriv_table(np.array([-1.0, 0.0, 1.0]))
DDC = (DC * DC).T


def diag3(flux):
    s = flux[0] + flux[2]
    return [
        DDC[0][0] * flux[0] + DDC[0][1] * flux[1] + DDC[0][2] * flux[2],
        DDC[1][0] * s,
        DDC[2][0] * flux[0] + DDC[2][1] * flux[1] + DDC[2][2] * flux[2],
    ]


def restrict5(y):
    return [y[0] + JA * y[1] + JC * y[3], JB * (y[1] + y[3]) + y[2], y[4] + JC * y[1] + JA * y[3]]


def up(x):
    return pltpu.roll(x, 127, 1)


def down(x):
    return pltpu.roll(x, 1, 1)


def loop(count, body):
    def step(i, carry):
        body(i)
        return carry

    lax.fori_loop(0, count, step, 0)


def unrolled(count, body):
    for i in range(count):
        body(i)


class Level:
    def __init__(self, q, fxy, f0, fq, mass, inv):
        self.q, self.kz = q, q - 1
        self.fxy, self.f0, self.fq, self.mass, self.inv = fxy, f0, fq, mass, inv
        self.stiff, self.diag = (stiff5, diag5) if q == 5 else (stiff3, diag3)
        self.face = q * self.kz * 4

    def at(self, i, j, k):
        return ((i * self.q + j) * self.kz + k) * 16

    def edge(self, i, j):
        return (i * self.q + j) * 16


def row(ref, start):
    if not isinstance(start, int):
        start = pl.multiple_of(start, 16)
    return ref[pl.ds(start, 16), :]


def put(ref, start, value):
    if not isinstance(start, int):
        start = pl.multiple_of(start, 16)
    ref[pl.ds(start, 16), :] = value


def element_rows():
    e = lax.broadcasted_iota(jnp.int32, (16, 128), 0)
    return e // 4, e % 4


def join_y(lo, hi):
    _, ey = element_rows()
    hi = hi + jnp.where(ey < 3, pltpu.roll(lo, 15, 0), 0.0)
    return jnp.where(ey > 0, pltpu.roll(hi, 1, 0), lo), hi


def join_x(lo, hi):
    ex, _ = element_rows()
    hi = hi + jnp.where(ex < 3, pltpu.roll(lo, 12, 0), 0.0)
    return jnp.where(ex > 0, pltpu.roll(hi, 4, 0), lo), hi


def join_planes_x(lv, out):
    q, kz = lv.q, lv.kz

    def body(j):
        for k in range(kz):
            lo, hi = join_x(row(out, lv.at(0, j, k)), row(out, lv.at(q - 1, j, k)))
            put(out, lv.at(0, j, k), lo)
            put(out, lv.at(q - 1, j, k), hi)

    unrolled(q, body)


def join_planes_y(lv, out):
    q, kz = lv.q, lv.kz

    def body(i):
        for k in range(kz):
            lo, hi = join_y(row(out, lv.at(i, 0, k)), row(out, lv.at(i, q - 1, k)))
            put(out, lv.at(i, 0, k), lo)
            put(out, lv.at(i, q - 1, k), hi)

    unrolled(q, body)


def apply_local(lv, out, u, scaled=None, sums=None, restrict=None, keep=True):
    q, kz = lv.q, lv.kz

    def along_z(i):
        total = None
        for j in range(q):
            base = lv.at(i, j, 0)
            if scaled is None:
                v = [row(u, base + 16 * k) for k in range(kz)]
            else:
                v = [row(scaled, base + 16 * k) * row(lv.inv, base + 16 * k) for k in range(kz)]
                for k in range(kz):
                    put(u, base + 16 * k, v[k])
                if sums is not None:
                    part = v[0] * v[0]
                    part = part + part
                    for k in range(1, kz):
                        part = part + v[k] * v[k]
                    total = part if total is None else total + part
            flux = [row(lv.f0, lv.edge(i, j))] + [row(lv.fxy, base + 16 * k) for k in range(1, kz)] + [row(lv.fq, lv.edge(i, j))]
            g = lv.stiff(v + [up(v[0])], flux)
            g = [g[0] + down(g[kz])] + g[1:kz]
            for k in range(kz):
                put(out, base + 16 * k, g[k] + row(lv.mass, base + 16 * k) * v[k])
        if sums is not None:
            sums[...] += total

    def along_x(j):
        for k in range(kz):
            places = [lv.at(i, j, k) for i in range(q)]
            g = lv.stiff([row(u, p) for p in places], [row(lv.fxy, p) for p in places])
            for i in range(q):
                put(out, places[i], row(out, places[i]) + g[i])

    def along_y(i):
        for k in range(kz):
            places = [lv.at(i, j, k) for j in range(q)]
            g = lv.stiff([row(u, p) for p in places], [row(lv.fxy, p) for p in places])
            g = [row(out, places[j]) + g[j] for j in range(q)]
            if restrict is not None:
                c = restrict5(g)
                for jc in range(3):
                    put(restrict, ((i * 3 + jc) * 4 + k) * 16, c[jc])
            if keep:
                g[0], g[q - 1] = join_y(g[0], g[q - 1])
                for j in range(q):
                    put(out, places[j], g[j])

    if sums is not None:
        sums[...] = jnp.zeros_like(sums)
    unrolled(q, along_z)
    unrolled(q, along_x)
    unrolled(q, along_y)
    if keep:
        join_planes_x(lv, out)


def sum_squares(lv, scaled, sums):
    total = [None] * 4
    for i in range(lv.q - 1):
        for j in range(lv.q - 1):
            for k in range(lv.kz):
                p = lv.at(i, j, k)
                v = row(scaled, p) * row(lv.inv, p)
                v = v * v
                zeros = (i == 0) + (j == 0) + (k == 0)
                total[zeros] = v if total[zeros] is None else total[zeros] + v
    sums[...] = total[0] + 2.0 * total[1] + 4.0 * total[2] + 8.0 * total[3]


def restrict_xz(lc, tmp, out):
    for jc in range(3):
        cols = [restrict5([row(tmp, ((i * 3 + jc) * 4 + k) * 16) for i in range(5)]) for k in range(4)]
        for ic in range(3):
            y = [cols[k][ic] for k in range(4)]
            first = y[0] + JA * y[1] + JC * y[3] + down(JC * y[1] + JA * y[3])
            put(out, lc.at(ic, jc, 0), first)
            put(out, lc.at(ic, jc, 1), JB * (y[1] + y[3]) + y[2])
    join_planes_y(lc, out)
    join_planes_x(lc, out)


def restrict_y(lv, src, tmp):
    def body(i):
        for k in range(4):
            c = restrict5([row(src, lv.at(i, j, k)) for j in range(5)])
            for jc in range(3):
                put(tmp, ((i * 3 + jc) * 4 + k) * 16, c[jc])

    unrolled(5, body)


def local_diag(lv, out):
    q, kz = lv.q, lv.kz

    def along_z(i):
        for j in range(q):
            base = lv.at(i, j, 0)
            flux = [row(lv.f0, lv.edge(i, j))] + [row(lv.fxy, base + 16 * k) for k in range(1, kz)] + [row(lv.fq, lv.edge(i, j))]
            g = lv.diag(flux)
            g = [g[0] + down(g[kz])] + g[1:kz]
            for k in range(kz):
                put(out, base + 16 * k, g[k] + row(lv.mass, base + 16 * k))

    def along_x(j):
        for k in range(kz):
            places = [lv.at(i, j, k) for i in range(q)]
            g = lv.diag([row(lv.fxy, p) for p in places])
            for i in range(q):
                put(out, places[i], row(out, places[i]) + g[i])

    def along_y(i):
        for k in range(kz):
            places = [lv.at(i, j, k) for j in range(q)]
            g = lv.diag([row(lv.fxy, p) for p in places])
            g = [row(out, places[j]) + g[j] for j in range(q)]
            g[0], g[q - 1] = join_y(g[0], g[q - 1])
            for j in range(q):
                put(out, places[j], g[j])

    unrolled(q, along_z)
    unrolled(q, along_x)
    unrolled(q, along_y)
    join_planes_x(lv, out)


DIRS = [(0, 1), (0, -1), (1, 0), (-1, 0), (1, 1), (1, -1), (-1, 1), (-1, -1)]


def directions(forward):
    return [d for d, (dx, dy) in enumerate(DIRS) if not forward or (dx >= 0 and dy >= 0)]


def wait_all(ref, sem):
    pltpu.make_async_copy(ref, ref, sem).wait()


class Exchange:
    def __init__(self, round_index, fields, region, bufs, sems, ids, forward):
        self.r, self.fields, self.ids = round_index, fields, ids
        self.bufs, self.sems = bufs, sems
        face, corner = sum(lv.face for lv, _ in fields), 8 * len(fields)
        self.dirs = directions(forward)
        self.part, at = {}, region[0]
        for d in self.dirs:
            self.part[d] = (at, face if d < 4 else corner)
            at += self.part[d][1]
        assert at == region[0] + region[1]
        self.region = pl.ds(*region)

    def pack(self):
        sbuf = self.bufs[0]
        at = 0
        for f, (lv, ref) in enumerate(self.fields):
            q, kz = lv.q, lv.kz
            for d, (dx, dy) in enumerate(DIRS[:4]):
                if d not in self.dirs:
                    continue
                if dy:
                    j, first = (q - 1, 3) if dy > 0 else (0, 0)
                    for i in range(q):
                        for h in range(0, 4 * kz, 8):
                            sbuf[pl.ds(self.part[d][0] + at + i * 4 * kz + h, 8), :] = ref[pl.ds(lv.at(i, j, 0) + first + 4 * h, 8, 4), :]
                else:
                    i = q - 1 if dx > 0 else 0
                    low = lax.broadcasted_iota(jnp.int32, (8, 128), 0) < 4
                    for m in range(0, q * kz, 2):
                        p = lv.at(i, 0, 0) + m * 16
                        if dx > 0:
                            one, two = ref[pl.ds(p + 8, 8), :], ref[pl.ds(p + 24, 8), :]
                            both = jnp.where(low, pltpu.roll(one, 4, 0), two)
                        else:
                            one, two = ref[pl.ds(p, 8), :], ref[pl.ds(p + 16, 8), :]
                            both = jnp.where(low, one, pltpu.roll(two, 4, 0))
                        sbuf[pl.ds(self.part[d][0] + at + m * 4, 8), :] = both
            for c, (dx, dy) in enumerate(DIRS[4:]):
                if c + 4 not in self.dirs:
                    continue
                p = lv.at(q - 1 if dx > 0 else 0, q - 1 if dy > 0 else 0, 0) + (12 if dx > 0 else 0) + (3 if dy > 0 else 0)
                for k in range(kz):
                    sbuf[pl.ds(self.part[c + 4][0] + f * 8 + k, 1), :] = ref[pl.ds(p + 16 * k, 1), :]
            at += lv.face

    def send(self):
        sbuf, rbuf = self.bufs
        send_sem, recv_sem = self.sems
        x, y, nx, ny = self.ids
        for d in self.dirs:
            dx, dy = DIRS[d]
            part = pl.ds(*self.part[d])
            pltpu.make_async_remote_copy(
                src_ref=sbuf.at[part],
                dst_ref=rbuf.at[part],
                send_sem=send_sem.at[self.r],
                recv_sem=recv_sem.at[self.r],
                device_id=(lax.rem(x + dx + nx, nx), lax.rem(y + dy + ny, ny)),
                device_id_type=MESH,
            ).start()

    def start(self):
        self.pack()
        self.send()

    def finish(self):
        rbuf = self.bufs[1]
        wait_all(rbuf.at[self.region], self.sems[1].at[self.r])
        at = 0
        for f, (lv, ref) in enumerate(self.fields):
            q, kz = lv.q, lv.kz
            for d, (dx, dy) in enumerate(DIRS[:4]):
                if d not in self.dirs:
                    continue
                if dy:
                    j, first = (0, 0) if dy > 0 else (q - 1, 3)
                    for i in range(q):
                        for h in range(0, 4 * kz, 8):
                            place = pl.ds(lv.at(i, j, 0) + first + 4 * h, 8, 4)
                            ref[place, :] = ref[place, :] + rbuf[pl.ds(self.part[d][0] + at + i * 4 * kz + h, 8), :]
                else:
                    i = 0 if dx > 0 else q - 1
                    low = lax.broadcasted_iota(jnp.int32, (8, 128), 0) < 4
                    for m in range(0, q * kz, 2):
                        p = lv.at(i, 0, 0) + m * 16
                        both = rbuf[pl.ds(self.part[d][0] + at + m * 4, 8), :]
                        turned = pltpu.roll(both, 4, 0)
                        if dx > 0:
                            a, b = pl.ds(p, 8), pl.ds(p + 16, 8)
                            ref[a, :] = ref[a, :] + jnp.where(low, both, 0.0)
                            ref[b, :] = ref[b, :] + jnp.where(low, turned, 0.0)
                        else:
                            a, b = pl.ds(p + 8, 8), pl.ds(p + 24, 8)
                            ref[a, :] = ref[a, :] + jnp.where(low, 0.0, turned)
                            ref[b, :] = ref[b, :] + jnp.where(low, 0.0, both)
            for c, (dx, dy) in enumerate(DIRS[4:]):
                if c + 4 not in self.dirs:
                    continue
                p = lv.at(0 if dx > 0 else q - 1, 0 if dy > 0 else q - 1, 0) + (0 if dx > 0 else 12) + (0 if dy > 0 else 3)
                for k in range(kz):
                    place = pl.ds(p + 16 * k, 1)
                    ref[place, :] = ref[place, :] + rbuf[pl.ds(self.part[c + 4][0] + f * 8 + k, 1), :]
            at += lv.face

    def wait_sent(self):
        wait_all(self.bufs[0].at[self.region], self.sems[0].at[self.r])


class Lanes:
    def __init__(self, q):
        self.q = q
        step = {k: (k - 128) % q for k in range(q)}
        shift = {0: 0}
        k = 0
        for _ in range(q - 1):
            shift[step[k]] = shift[k] + self.begin(k, 1) - self.begin(step[k], 0)
            k = step[k]
        self.shift = [shift[k] % 128 for k in range(q)]
        lane = lax.broadcasted_iota(jnp.int32, (8, 128), 1)
        self.lane = lane
        self.split_index, self.merge_index = [], []
        for t in range(q):
            place = 128 * t + lane
            k = lax.rem(place, q)
            ez = lax.div(place, q)
            moved = ez
            for node in range(q):
                moved = jnp.where(k == node, ez + self.shift[node], moved)
            self.merge_index.append(jnp.bitwise_and(moved, 127))
            index = jnp.zeros((8, 128), jnp.int32)
            for node in range(q):
                ez = jnp.bitwise_and(lane - self.shift[node] + 128, 127)
                index = jnp.where(self.inside(node, t), q * ez + node - 128 * t, index)
            self.split_index.append(index)

    def begin(self, k, t):
        return -((k - 128 * t) // self.q)

    def inside(self, k, t):
        lo, hi = (self.begin(k, t) + self.shift[k]) % 128, (self.begin(k, t + 1) + self.shift[k]) % 128
        if lo < hi:
            return (self.lane >= lo) & (self.lane < hi) if lo else self.lane < hi
        return (self.lane >= lo) | (self.lane < hi) if hi else self.lane >= lo

    @staticmethod
    def gather(x, index):
        numbers = lax.GatherDimensionNumbers(
            offset_dims=(), collapsed_slice_dims=(1,), start_index_map=(1,), operand_batching_dims=(0,), start_indices_batching_dims=(0,)
        )
        return lax.gather(x, index[..., None], numbers, slice_sizes=(1, 1), mode=lax.GatherScatterMode.PROMISE_IN_BOUNDS)

    def unmix(self, moved):
        out = []
        for k in range(self.q):
            x = moved[0]
            for t in range(1, self.q):
                x = jnp.where(self.inside(k, t), moved[t], x)
            out.append(pltpu.roll(x, (128 - self.shift[k]) % 128, 1) if self.shift[k] else x)
        return out

    def mix(self, nodes):
        moved = [pltpu.roll(nodes[k], self.shift[k], 1) if self.shift[k] else nodes[k] for k in range(self.q)]
        out = []
        for t in range(self.q):
            x = moved[0]
            for k in range(1, self.q):
                x = jnp.where(self.inside(k, t), moved[k], x)
            out.append(x)
        return out


def pick(i, values):
    out = jnp.asarray(values[-1], F32)
    for n in range(len(values) - 2, -1, -1):
        out = jnp.where(i == n, jnp.asarray(values[n], F32), out)
    return out


def load_field(lanes, ref, raw, index, buf, sem, store):
    def tile(t):
        pltpu.make_async_copy(ref.at[:, :, pl.ds(pl.multiple_of(128 * t, 128), 128)], raw.at[t], sem.at[t]).wait()
        order = index[t]
        for i in range(5):
            for j in range(5):
                for h in range(2):
                    low = raw[t, 10 * h + i, pl.ds(j, 4, 5), :]
                    high = raw[t, 10 * h + 5 + i, pl.ds(j, 4, 5), :]
                    both = jnp.concatenate([low, high], axis=0)
                    buf[t, pl.ds((i * 5 + j) * 16 + 8 * h, 8), :] = lanes.gather(both, order)

    def plane(i):
        wx = pick(i, WF)
        for j in range(5):
            halves = []
            for h in range(2):
                p = pl.ds(pl.multiple_of((i * 5 + j) * 16 + 8 * h, 8), 8)
                halves.append(lanes.unmix([buf[t, p, :] for t in range(5)]))
            store(i, j, [jnp.concatenate([halves[0][k], halves[1][k]], axis=0) * (wx * (WF[j] * WF[k])) for k in range(5)])

    loop(5, tile)
    loop(5, plane)


FR, CR, ER, CER = 1600, 288, 400, 144


def cheb_weights():
    sigma, rho = 5.0 / 3.0, 0.6
    theta, delta = 0.75, 0.45
    d = np.array([1.0 / theta, 0.0, 0.0])
    x = np.zeros(3)
    for sweep in range(SWEEPS):
        x = x + d
        if sweep + 1 < SWEEPS:
            nxt = 1.0 / (2.0 * sigma - rho)
            res = np.array([1.0, 0.0, 0.0]) - np.concatenate([[0.0], x[:-1]])
            d = nxt * rho * d + 2.0 * nxt / delta * res
            rho = nxt
    return [float(c) for c in x]


CHEB = cheb_weights()

ROUNDS = [
    (1, 0, False), (1, 0, False), (0, 2, False), (1, 0, False), (1, 0, False), (0, 1, False), (1, 0, True), (0, 2, False),
    (0, 1, True), (1, 0, False), (0, 1, False), (0, 1, False), (0, 2, False), (0, 1, False), (0, 1, False),
]


def round_regions():
    at, out = 0, []
    for fine, coarse, forward in ROUNDS:
        sizes = [80 * fine + 24 * coarse if d < 4 else 8 * (fine + coarse) for d in directions(forward)]
        out.append((at, sum(sizes)))
        at += sum(sizes)
    return out, at


REGIONS, BUF_ROWS = round_regions()


def kernel(nx, ny, src, cond, absn, smooth_ref, corr, merge_index, *s):
    (raw, gbuf, split_index, fxy, f0, f4, mass, inv, load, u0, u1, u2, pa, first, pb, ca, cb, last, tmp,
     cfxy, cf0, cf2, cmass, cinv, rl, cfirst, qa, qb, ra0, ra1, ra2, vl, v0, v1, v2, al, a0, a1, a2, w0, w1, wa, wc, base,
     s1, s2, s3, s4, ar1, ar2, arx, ary, sbuf, rbuf, in_sem, send_sem, recv_sem, ar_send, ar_recv) = s
    x, y = lax.axis_index("gx"), lax.axis_index("gy")

    for a, ref in enumerate((src, cond, absn)):
        for t in range(5):
            pltpu.make_async_copy(ref.at[:, :, pl.ds(128 * t, 128)], raw.at[a, t], in_sem.at[a, t]).start()

    def x_peer(d):
        return (lax.rem(x + d + nx, nx), y)

    def y_peer(d):
        return (x, lax.rem(y + d + ny, ny))

    barrier = pltpu.get_barrier_semaphore()
    greeted = [(lax.rem(x + dx + nx, nx), lax.rem(y + dy + ny, ny)) for dx, dy in DIRS[4:]]
    greeted += [x_peer(d) for d in range(1, nx)] + [y_peer(d) for d in range(1, ny)]
    for peer in greeted:
        pl.semaphore_signal(barrier, inc=1, device_id=peer, device_id_type=MESH)

    lf = Level(5, fxy, f0, f4, mass, inv)
    lc = Level(3, cfxy, cf0, cf2, cmass, cinv)
    bufs, sems, ids = (sbuf, rbuf), (send_sem, recv_sem), (x, y, nx, ny)
    rounds = []

    def exchange(index, *fields, forward=False):
        e = Exchange(index, fields, REGIONS[index], bufs, sems, ids, forward)
        e.start()
        if len(rounds) >= 4:
            rounds[-4].wait_sent()
        rounds.append(e)
        return e

    lanes = Lanes(5)
    for t in range(5):
        split_index[t] = lanes.split_index[t]
        merge_index[t] = lanes.merge_index[t]

    def read(a, ref, store):
        load_field(lanes, ref, raw.at[a], split_index, gbuf, in_sem.at[a], store)

    def store_flux(i, j, p):
        put(f0, lf.edge(i, j), p[0])
        put(f4, lf.edge(i, j), p[4])
        put(fxy, lf.at(i, j, 0), p[0] + down(p[4]))
        for k in range(1, 4):
            put(fxy, lf.at(i, j, k), p[k])

    def store_plain(ref):
        def store(i, j, p):
            put(ref, lf.at(i, j, 0), p[0] + down(p[4]))
            for k in range(1, 4):
                put(ref, lf.at(i, j, k), p[k])

        return store

    read(0, src, store_plain(load))
    restrict_y(lf, load, tmp)
    join_planes_y(lf, load)
    join_planes_x(lf, load)
    restrict_xz(lc, tmp, rl)
    read(1, cond, store_flux)
    pl.semaphore_wait(barrier, len(greeted))
    e_load = exchange(0, (lf, load))
    read(2, absn, store_plain(mass))
    for i in range(3):
        for j in range(3):
            ratio = WC[i] * WC[j] / (WF[2 * i] * WF[2 * j])
            ends, mid = ratio * WC[0] / WF[0], ratio * WC[1] / WF[2]
            put(cf0, lc.edge(i, j), ends * row(f0, lf.edge(2 * i, 2 * j)))
            put(cf2, lc.edge(i, j), ends * row(f4, lf.edge(2 * i, 2 * j)))
            for a, b in ((cfxy, fxy), (cmass, mass)):
                put(a, lc.at(i, j, 0), ends * row(b, lf.at(2 * i, 2 * j, 0)))
                put(a, lc.at(i, j, 1), mid * row(b, lf.at(2 * i, 2 * j, 2)))
    local_diag(lf, inv)
    e_diag = exchange(1, (lf, inv))
    local_diag(lc, cinv)
    e_coarse = exchange(2, (lc, rl), (lc, cinv))

    def invert(lv):
        def body(i):
            for n in range(lv.q * lv.kz):
                p = lv.at(i, 0, 0) + n * 16
                put(lv.inv, p, 1.0 / row(lv.inv, p))

        unrolled(lv.q, body)

    e_load.finish()
    apply_local(lf, pa, load)
    e_pa = exchange(3, (lf, pa))
    e_diag.finish()
    invert(lf)
    apply_local(lf, ca, u0, scaled=load, restrict=tmp)
    e_ca = exchange(4, (lf, ca))
    restrict_xz(lc, tmp, ra0)
    e_coarse.finish()
    invert(lc)
    apply_local(lc, qa, rl)
    e_qa = exchange(5, (lc, qa))
    apply_local(lc, al, vl, scaled=rl)
    e_pa.finish()
    apply_local(lf, pb, first, scaled=pa, sums=s1)
    e_pb = exchange(6, (lf, pb), forward=True)
    e_al = exchange(7, (lc, ra0), (lc, al))
    e_qa.finish()
    apply_local(lc, qb, cfirst, scaled=qa, sums=s3)
    e_qb = exchange(8, (lc, qb), forward=True)
    e_ca.finish()
    apply_local(lf, cb, u1, scaled=ca, restrict=tmp)
    e_cb = exchange(9, (lf, cb))
    restrict_xz(lc, tmp, ra1)
    e_pb.finish()
    sum_squares(lf, pb, s2)
    e_qb.finish()
    sum_squares(lc, qb, s4)

    def fold(sums):
        return jnp.sum(sums[...], axis=0, keepdims=True)

    def to_all(phase, source, slots, count, peer):
        for d in range(1, count):
            pltpu.make_async_remote_copy(
                src_ref=source,
                dst_ref=slots.at[d],
                send_sem=ar_send.at[phase],
                recv_sem=ar_recv.at[phase],
                device_id=peer(d),
                device_id_type=MESH,
            ).start()

    def gathered(phase, source, slots, count):
        wait_all(slots.at[pl.ds(1, count - 1)], ar_recv.at[phase])
        total = source[...]
        for d in range(1, count):
            total = total + slots[d]
        wait_all(slots.at[pl.ds(1, count - 1)], ar_send.at[phase])
        return total

    ar1[...] = jnp.concatenate([fold(s1), fold(s2), fold(s3), fold(s4), jnp.zeros((4, 128), F32)], axis=0)
    to_all(0, ar1, arx, nx, x_peer)
    e_ra1 = exchange(10, (lc, ra1))
    e_al.finish()
    apply_local(lc, a0, v0, scaled=ra0)

    e_cb.finish()
    apply_local(lf, last, u2, scaled=cb, restrict=tmp, keep=False)
    restrict_xz(lc, tmp, ra2)
    e_ra2 = exchange(11, (lc, ra2))
    e_ra1.finish()
    apply_local(lc, a1, v1, scaled=ra1)
    ar2[...] = gathered(0, ar1, arx, nx)
    to_all(1, ar2, ary, ny, y_peer)
    e_a01 = exchange(12, (lc, a0), (lc, a1))
    e_ra2.finish()
    apply_local(lc, a2, v2, scaled=ra2)
    e_a2 = exchange(13, (lc, a2))
    e_a01.finish()
    totals = jnp.sum(gathered(1, ar2, ary, ny), axis=1, keepdims=True)

    def inverse_estimate(n):
        estimate = jnp.sqrt(totals[n + 1 : n + 2] / (totals[n : n + 1] + 1e-06))
        return jnp.broadcast_to(1.0 / estimate, (16, 128))

    g, gc = inverse_estimate(0), inverse_estimate(2)

    def horner(scale, a, b, c):
        return scale * (CHEB[0] * a + scale * (CHEB[1] * b + scale * (CHEB[2] * c)))

    for n in range(18):
        p = 16 * n
        put(w0, p, row(vl, p) - horner(g, row(v0, p), row(v1, p), row(v2, p)))
        put(wa, p, row(al, p) - g * (CHEB[0] * row(a0, p) + g * (CHEB[1] * row(a1, p))))

    def smooth(i):
        for n in range(20):
            p = lf.at(i, 0, 0) + 16 * n
            put(smooth_ref, p, horner(g, row(u0, p), row(u1, p), row(u2, p)))

    loop(5, smooth)
    e_a2.finish()
    for n in range(18):
        p = 16 * n
        put(wa, p, row(wa, p) - g * (g * (g * (CHEB[2] * row(a2, p)))))
    apply_local(lc, wc, w1, scaled=wa)
    e_w1 = exchange(14, (lc, wc))
    for n in range(18):
        p = 16 * n
        put(base, p, gc * (CHEB[0] * row(w0, p) + gc * (CHEB[1] * row(w1, p))))
    e_w1.finish()
    for n in range(18):
        p = 16 * n
        put(corr, p, row(base, p) + gc * (gc * (gc * (CHEB[2] * row(wc, p) * row(cinv, p)))))

    for e in rounds[-4:]:
        e.wait_sent()


def lift(smooth_ref, corr, merge_index, out_ref, corr_ref, gbuf, obuf, cbuf, tmp, out_sem, cout_sem):
    lanes = Lanes(5)

    thirds = Lanes(3)
    for i in range(3):
        for j in range(3):
            c = [row(corr, ((i * 3 + j) * 2) * 16), row(corr, ((i * 3 + j) * 2 + 1) * 16)]
            c.append(up(c[0]))
            for h in range(2):
                for t, v in enumerate(thirds.mix([v[8 * h : 8 * h + 8] for v in c])):
                    stored = thirds.gather(v, thirds.merge_index[t])
                    cbuf[t, 6 * h + i, pl.ds(j, 4, 3), :] = stored[:4]
                    cbuf[t, 6 * h + 3 + i, pl.ds(j, 4, 3), :] = stored[4:]
    copies = []
    for t in range(3):
        copy = pltpu.make_async_copy(cbuf.at[t], corr_ref.at[:, :, pl.ds(128 * t, 128)], cout_sem.at[t])
        copy.start()
        copies.append(copy)

    for i in range(3):
        lines = []
        for j in range(3):
            a, b = row(corr, ((i * 3 + j) * 2) * 16), row(corr, ((i * 3 + j) * 2 + 1) * 16)
            c = up(a)
            lines.append([a, JA * a + JB * b + JC * c, b, JC * a + JB * b + JA * c])
        for k in range(4):
            a, b, c = lines[0][k], lines[1][k], lines[2][k]
            for j, v in enumerate([a, JA * a + JB * b + JC * c, b, JC * a + JB * b + JA * c, c]):
                put(tmp, ((i * 5 + j) * 4 + k) * 16, v)

    def finish_plane(i):
        cx = [pick(i, [r[c] for r in JROWS]) for c in range(3)]
        for j in range(5):
            planes = []
            for k in range(4):
                lifted = [row(tmp, ((c * 5 + j) * 4 + k) * 16) for c in range(3)]
                lifted = cx[0] * lifted[0] + cx[1] * lifted[1] + cx[2] * lifted[2]
                planes.append(row(smooth_ref, ((i * 5 + j) * 4 + k) * 16) + lifted)
            planes.append(up(planes[0]))
            for h in range(2):
                for t, v in enumerate(lanes.mix([v[8 * h : 8 * h + 8] for v in planes])):
                    gbuf[t, pl.ds(pl.multiple_of((i * 5 + j) * 16 + 8 * h, 8), 8), :] = v

    def out_copy(t):
        return pltpu.make_async_copy(obuf.at[t], out_ref.at[:, :, pl.ds(pl.multiple_of(128 * t, 128), 128)], out_sem.at[t])

    def finish_tile(t):
        order = merge_index[t]
        for i in range(5):
            for j in range(5):
                for h in range(2):
                    stored = lanes.gather(gbuf[t, pl.ds((i * 5 + j) * 16 + 8 * h, 8), :], order)
                    obuf[t, 10 * h + i, pl.ds(j, 4, 5), :] = stored[:4]
                    obuf[t, 10 * h + 5 + i, pl.ds(j, 4, 5), :] = stored[4:]
        out_copy(t).start()

    loop(5, finish_plane)
    loop(5, finish_tile)

    copies += [out_copy(t) for t in range(5)]
    for copy in copies:
        copy.wait()


def scratch(nx, ny):
    def v(*shape):
        return pltpu.VMEM(shape, F32)

    fine, coarse = v(FR, 128), v(CR, 128)
    dma = pltpu.SemaphoreType.DMA
    return (
        [v(3, 5, 20, 20, 128), v(5, 400, 128), pltpu.VMEM((5, 8, 128), jnp.int32)]
        + [fine, v(ER, 128), v(ER, 128)]
        + [fine] * 12
        + [v(960, 128)]
        + [coarse, v(CER, 128), v(CER, 128)]
        + [coarse] * 22
        + [v(16, 128)] * 4
        + [v(8, 128), v(8, 128), v(nx, 8, 128), v(ny, 8, 128)]
        + [v(BUF_ROWS, 128)] * 2
        + [dma((3, 5)), dma((len(ROUNDS),)), dma((len(ROUNDS),)), dma((2,)), dma((2,))]
    )


def solution(mesh):
    nx, ny = mesh.shape["gx"], mesh.shape["gy"]

    def on_device(source, conductivity, absorption):
        vmem, hbm = pl.BlockSpec(memory_space=pltpu.VMEM), pl.BlockSpec(memory_space=pltpu.HBM)
        parts = pl.pallas_call(
            functools.partial(kernel, nx, ny),
            out_shape=(jax.ShapeDtypeStruct((FR, 128), F32), jax.ShapeDtypeStruct((CR, 128), F32), jax.ShapeDtypeStruct((5, 8, 128), jnp.int32)),
            in_specs=[hbm] * 3,
            out_specs=[vmem] * 3,
            scratch_shapes=scratch(nx, ny),
            compiler_params=pltpu.CompilerParams(collective_id=0, has_side_effects=True, vmem_limit_bytes=105 * 512 * 1024),
            name="window",
        )(source, conductivity, absorption)
        return pl.pallas_call(
            lift,
            out_shape=(jax.ShapeDtypeStruct((20, 20, 640), F32), jax.ShapeDtypeStruct((12, 12, 384), F32)),
            in_specs=[vmem] * 3,
            out_specs=[hbm] * 2,
            scratch_shapes=[
                pltpu.VMEM((5, 400, 128), F32),
                pltpu.VMEM((5, 20, 20, 128), F32),
                pltpu.VMEM((3, 12, 12, 128), F32),
                pltpu.VMEM((960, 128), F32),
                pltpu.SemaphoreType.DMA((5,)),
                pltpu.SemaphoreType.DMA((3,)),
            ],
            compiler_params=pltpu.CompilerParams(vmem_limit_bytes=16 * 1024 * 1024),
            name="lift",
        )(*parts)

    placed = P("gx", "gy", None)
    return jax.shard_map(on_device, mesh=mesh, in_specs=(placed,) * 3, out_specs=(placed, placed), check_vma=False)
```
